32 devices in a mesh: group: 4 (over x, core), tile: 8 (over z, y).
Axes of the slice: x: 2, y: 2, z: 4, core: 2. Of those that a mesh axis runs over, the one named last changes fastest.
Arguments:
- tokens: bfloat16 [64, 256, 128], P('group', 'tile'), may hold values from -6 to 6
- gain1: float32 [128], replicated, may hold values from 0.25 to 1.75
- w_qkv: bfloat16 [128, 384], replicated, may hold values from -0.5 to 0.5
- w_proj: bfloat16 [128, 128], replicated, may hold values from -0.5 to 0.5
- bias_table: float32 [4, 31, 31], replicated, may hold values from -70 to 150
- gain2: float32 [128], replicated, may hold values from 0.25 to 1.75
- w_fc1: bfloat16 [128, 512], replicated, may hold values from -0.5 to 0.5
- w_fc2: bfloat16 [512, 128], replicated, may hold values from -0.25 to 0.25
- cotangent: bfloat16 [64, 256, 128], P('group', 'tile'), may hold values from -6 to 6
Outputs:
- block_output: bfloat16 [64, 256, 128], P('group', 'tile')
- grad_tokens: bfloat16 [64, 256, 128], P('group', 'tile')
- grad_gain1: float32 [128], replicated
- grad_qkv: float32 [128, 384], replicated
- grad_proj: float32 [128, 128], replicated
- grad_table: float32 [4, 31, 31], replicated
- grad_gain2: float32 [128], replicated
- grad_fc1: float32 [128, 512], replicated
- grad_fc2: float32 [512, 128], replicated
The draws below stay inside these ranges and needn't reach their ends.
All inputs are finite; a program needn't handle non-finite values.
Results may differ from the reference program's by a relative error of at most 0.019.
Values may be sent and summed in bfloat16 or wider, within the bound.
No kernel may reach another device: no remote copies, remote signals or barrier semaphores. Data moves between devices by JAX's collectives and lax.ppermute only.
A program may use at most 64 MiB of HBM per device.

```python
import math
import jax
import jax.numpy as jnp
from jax import lax

C = 128
HEADS = 4
FF = 512
WIN = 16
ROWS_DEV = 16
COLS_DEV = 32
SHIFT = 8
HEIGHT = 64
WIDTH = 256
TOKENS = 16384


def draw_bias_table(key, part):
    table_shape = (HEADS, 2 * WIN - 1, 2 * WIN - 1)
    return jax.random.normal(key, table_shape, jnp.float32)


def block_levels(stream_key, dims, shards, smallest, high):
    def one(dim, shards_of):
        heights = jax.random.uniform(jax.random.fold_in(jax.random.fold_in(stream_key, 6), dim), (shards_of,), jnp.float32, smallest / len(shards), high / len(shards))
        return jnp.repeat(jnp.exp(heights), dims[dim] // shards_of).reshape((-1,) + (1,) * (len(dims) - dim - 1))

    gain = one(*shards[0])
    for cut in shards[1:]:
        gain = gain * one(*cut)
    return gain


def scatter_about(own_key, shape, width, bound, shards=(), held_as=jnp.bfloat16):
    array = jax.random.normal(own_key, shape, jnp.float32) * width
    if len(shards) > 0:
        array = block_levels(own_key, shape, shards, -0.22, 0.18) * array
    return jnp.clip(array, min=-bound, max=bound).astype(held_as)


def setup_inputs(seed: int = 0) -> dict:
    streams_of = jax.random.split(jax.random.key(seed), 10)
    tokens = scatter_about(streams_of[0], (HEIGHT, WIDTH, C), 1.0, 6.0, ((0, 4), (1, 8)))
    gain1 = jnp.clip(1.0 + 0.15 * jax.random.normal(streams_of[1], (C,), jnp.float32), 0.25, 1.75)
    w_qkv = scatter_about(streams_of[2], (C, 3 * C), C ** -0.5, 0.5)
    w_proj = scatter_about(streams_of[3], (C, C), C ** -0.5, 0.5)
    bias_table = draw_bias_table(jax.random.fold_in(streams_of[9], 71), 0)
    gain2 = jnp.clip(1.0 + 0.15 * jax.random.normal(streams_of[5], (C,), jnp.float32), 0.25, 1.75)
    w_fc1 = scatter_about(streams_of[6], (C, FF), C ** -0.5, 0.5)
    w_fc2 = scatter_about(streams_of[7], (FF, C), FF ** -0.5, 0.25)
    cotangent = scatter_about(streams_of[8], (HEIGHT, WIDTH, C), 1.0, 6.0, ((0, 4), (1, 8)))
    return dict(tokens=tokens, gain1=gain1, w_qkv=w_qkv, w_proj=w_proj, bias_table=bias_table, gain2=gain2, w_fc1=w_fc1, w_fc2=w_fc2, cotangent=cotangent)


NORM_EPS = 1e-05

def layer_norm(values, gain_vector):
    average = lax.optimization_barrier(jnp.mean(values, axis=-1, keepdims=True))
    centred = values - average
    variance = lax.optimization_barrier(jnp.mean(centred * centred, axis=-1, keepdims=True))
    return centred * lax.rsqrt(variance + NORM_EPS) * gain_vector

def region_of(position, extent, window, half_window):
    return (position >= extent - window).astype(jnp.int32) + (position >= extent - half_window).astype(jnp.int32)

def offset_onehot(window):
    positions = jnp.arange(window, dtype=jnp.int32)
    offsets = positions[:, None] - positions[None, :] + window - 1
    return (offsets[:, :, None] == jnp.arange(2 * window - 1, dtype=jnp.int32)[None, None, :]).astype(jnp.float32)

def position_bias(bias_table, window):
    onehot = offset_onehot(window)
    partial_bias = jnp.einsum('hab,xzb->haxz', bias_table, onehot, precision=lax.Precision.HIGHEST)
    expanded = jnp.einsum('ywa,haxz->hyxwz', onehot, partial_bias, precision=lax.Precision.HIGHEST)
    return expanded.reshape(bias_table.shape[0], window * window, window * window)

def to_windows(tile_block, window):
    row_count, col_count = (tile_block.shape[0], tile_block.shape[1])
    trailing = tile_block.shape[2:]
    reshaped = tile_block.reshape((row_count // window, window, col_count // window, window) + trailing)
    order_axes = (0, 2, 1, 3) + tuple(range(4, 4 + len(trailing)))
    return reshaped.transpose(order_axes).reshape((row_count // window * (col_count // window), window * window) + trailing)

def from_windows(windows, row_count, col_count, window):
    trailing = windows.shape[2:]
    reshaped = windows.reshape((row_count // window, col_count // window, window, window) + trailing)
    order_axes = (0, 2, 1, 3) + tuple(range(4, 4 + len(trailing)))
    return reshaped.transpose(order_axes).reshape((row_count, col_count) + trailing)

def grid_blocks(grid, row_count, col_count):
    trailing = grid.shape[2:]
    reshaped = grid.reshape((grid.shape[0] // row_count, row_count, grid.shape[1] // col_count, col_count) + trailing)
    order_axes = (0, 2, 1, 3) + tuple(range(4, 4 + len(trailing)))
    return reshaped.transpose(order_axes).reshape((-1, row_count, col_count) + trailing)

def grid_merge(blocks, grid_height, grid_width):
    row_count, col_count = (blocks.shape[1], blocks.shape[2])
    trailing = blocks.shape[3:]
    reshaped = blocks.reshape((grid_height // row_count, grid_width // col_count, row_count, col_count) + trailing)
    order_axes = (0, 2, 1, 3) + tuple(range(4, 4 + len(trailing)))
    return reshaped.transpose(order_axes).reshape((grid_height, grid_width) + trailing)

def group_size(window_total, window_tokens):
    chosen = 1
    for candidate in range(1, window_total + 1):
        if window_total % candidate == 0 and candidate * window_tokens <= 512:
            chosen = candidate
    return chosen

def window_group(members, region_ids, w_qkv, w_proj, bias_values):
    window_count, window_tokens, feature_width = members.shape
    head_count = bias_values.shape[0]
    head_size = feature_width // head_count
    flattened = members.reshape(window_count * window_tokens, feature_width)
    projected = jnp.dot(flattened, w_qkv.astype(jnp.bfloat16), preferred_element_type=jnp.float32).astype(jnp.bfloat16)
    projected = projected.reshape(window_count, window_tokens, 3, head_count, head_size)
    queries = projected[:, :, 0].astype(jnp.float32)
    key_rows = projected[:, :, 1].astype(jnp.float32)
    value_rows = projected[:, :, 2].astype(jnp.float32)
    scores = jnp.einsum('bqhd,bkhd->bhqk', queries, key_rows, precision=lax.Precision.HIGHEST) * head_size ** (-0.5)
    scores = scores + bias_values[None]
    allowed = region_ids[:, None, :, None] == region_ids[:, None, None, :]
    scores = jnp.where(allowed, scores, -1e+30)
    row_max = lax.stop_gradient(lax.optimization_barrier(jnp.max(scores, axis=-1, keepdims=True)))
    exponent = jnp.exp(scores - row_max)
    softmax_weights = (exponent / lax.optimization_barrier(jnp.sum(exponent, axis=-1, keepdims=True))).astype(jnp.bfloat16)
    head_output = jnp.einsum('bhqk,bkhd->bqhd', softmax_weights.astype(jnp.float32), value_rows, precision=lax.Precision.HIGHEST).astype(jnp.bfloat16)
    result = jnp.dot(head_output.reshape(window_count * window_tokens, feature_width), w_proj.astype(jnp.bfloat16), preferred_element_type=jnp.float32)
    return result.astype(jnp.bfloat16).reshape(window_count, window_tokens, feature_width)

def feed_forward(hidden, gain2, w_fc1, w_fc2):
    normed_two = layer_norm(hidden, gain2).astype(jnp.bfloat16)
    flattened = normed_two.reshape(-1, normed_two.shape[-1])
    inner_units = jax.nn.gelu(jnp.dot(flattened, w_fc1.astype(jnp.bfloat16), preferred_element_type=jnp.float32), approximate=False).astype(jnp.bfloat16)
    output_rows = jnp.dot(inner_units, w_fc2.astype(jnp.bfloat16), preferred_element_type=jnp.float32)
    return (hidden + output_rows.reshape(hidden.shape)).astype(jnp.bfloat16)

def forward(tokens, gain1, w_qkv, w_proj, bias_table, gain2, w_fc1, w_fc2):
    residual_in = tokens.astype(jnp.float32)
    normed = layer_norm(residual_in, gain1).astype(jnp.bfloat16)
    shifted = jnp.roll(normed, (-SHIFT, -SHIFT), (0, 1))
    row_ids = jnp.arange(HEIGHT, dtype=jnp.int32)
    col_ids = jnp.arange(WIDTH, dtype=jnp.int32)
    region = 3 * region_of(row_ids, HEIGHT, WIN, SHIFT)[:, None] + region_of(col_ids, WIDTH, WIN, SHIFT)[None, :]
    bias_values = position_bias(bias_table, WIN)
    data_tiles = grid_blocks(shifted, ROWS_DEV, COLS_DEV)
    region_tiles = grid_blocks(region, ROWS_DEV, COLS_DEV)
    data_windows = jax.vmap(lambda piece: to_windows(piece, WIN))(data_tiles)
    region_windows = jax.vmap(lambda piece: to_windows(piece, WIN))(region_tiles)
    tile_count, window_total, window_tokens = (data_windows.shape[0], data_windows.shape[1], data_windows.shape[2])
    per_group = group_size(window_total, window_tokens)
    data_groups = data_windows.reshape(-1, per_group, window_tokens, C)
    region_groups = region_windows.reshape(-1, per_group, window_tokens)

    def attend_group(members):
        return window_group(members[0], members[1], w_qkv, w_proj, bias_values)
    attended = lax.map(jax.checkpoint(attend_group), (data_groups, region_groups))
    attended = attended.reshape(tile_count, window_total, window_tokens, C)
    attended = jax.vmap(lambda piece: from_windows(piece, ROWS_DEV, COLS_DEV, WIN))(attended)
    attended = grid_merge(attended, HEIGHT, WIDTH)
    returned = jnp.roll(attended, (SHIFT, SHIFT), (0, 1))
    hidden = residual_in + returned.astype(jnp.float32)

    def mlp_tile(hidden_tile):
        return feed_forward(hidden_tile, gain2, w_fc1, w_fc2)
    outputs = lax.map(jax.checkpoint(mlp_tile), grid_blocks(hidden, ROWS_DEV, COLS_DEV))
    return grid_merge(outputs, HEIGHT, WIDTH)

def reference(tokens, gain1, w_qkv, w_proj, bias_table, gain2, w_fc1, w_fc2, cotangent):
    block_output, pullback = jax.vjp(forward, tokens, gain1, w_qkv.astype(jnp.float32), w_proj.astype(jnp.float32), bias_table, gain2, w_fc1.astype(jnp.float32), w_fc2.astype(jnp.float32))
    grads = pullback(cotangent)
    grad_scale = 1.0 / math.sqrt(TOKENS)
    return (block_output, grads[0], grads[1] * grad_scale, grads[2] * grad_scale, grads[3] * grad_scale, grads[4] * grad_scale, grads[5] * grad_scale, grads[6] * grad_scale, grads[7] * grad_scale)
```

```python
import functools
import math

import jax
import jax.numpy as jnp
from jax import lax
from jax.experimental import pallas as pl
from jax.experimental.pallas import tpu as pltpu
from jax.sharding import PartitionSpec as P

WIN = 16
SHIFT = 8
NORM_EPS = 1e-05
LANES = 128
F32 = jnp.float32
BF16 = jnp.bfloat16
AXES = ("group", "tile")


def dot(left, right, left_dim, right_dim, precision=None):
    return lax.dot_general(
        left,
        right,
        (((left_dim,), (right_dim,)), ((), ())),
        preferred_element_type=F32,
        precision=precision,
    )


def iota(shape, dim):
    return lax.broadcasted_iota(jnp.int32, shape, dim)


def shift_rows(values, amounts, right):
    width = values.shape[1]
    for bit in range(4):
        step = 1 << bit
        moved = pltpu.roll(values, step if right else width - step, 1)
        values = jnp.where((amounts & step) != 0, moved, values)
    return values


def bias_kernel(heads, windows, flags_ref, table_ref, out_ref):
    span = 2 * WIN * WIN
    tokens = WIN * WIN
    offsets = 2 * WIN - 1
    lane = iota((offsets, span), 1)
    row = iota((offsets, span), 0)
    flats = []
    for odd in range(2):
        pick = jnp.where(lane % 32 == offsets - 1 - row, 1.0, 0.0).astype(F32)
        keep = (lane // 32) * 2 + odd == offsets - 1 - row
        for head in range(heads):
            spread = dot(table_ref[head], pick, 1, 0, lax.Precision.HIGHEST)
            flat = jnp.sum(jnp.where(keep, spread, 0.0), axis=0, keepdims=True)
            flats.append(jnp.broadcast_to(flat, (WIN, span)))
    rows = heads * WIN
    amounts = WIN - 1 - iota((rows, span), 0) % WIN
    even = shift_rows(jnp.concatenate(flats[:heads], 0), amounts, False)
    odd = shift_rows(jnp.concatenate(flats[heads:], 0), amounts, False)
    odd = pltpu.roll(odd, WIN, 1)
    strip = jnp.where(iota((rows, span), 1) % 32 < WIN, even, odd)
    last_row = flags_ref[0]
    last_col = flags_ref[1]
    key = iota((WIN, tokens), 1)
    query_x = iota((WIN, tokens), 0)
    key_low = (key >= tokens // 2).astype(jnp.int32)
    cross_col = ((key % WIN >= SHIFT) != (query_x >= SHIFT)).astype(jnp.int32)
    for fine in range(8):
        moved = pltpu.roll(strip, (span - WIN * fine) % span, 1)
        for coarse in range(2):
            y = WIN - 1 - (8 * coarse + fine)
            cross_row = key_low if y < SHIFT else 1 - key_low
            for window in range(windows):
                apart = cross_row * last_row
                if window == windows - 1:
                    apart = apart + cross_col * last_col
                extra = jnp.where(apart > 0, -1e30, 0.0)
                for head in range(heads):
                    part = moved[
                        head * WIN : (head + 1) * WIN,
                        LANES * coarse : LANES * coarse + tokens,
                    ]
                    start = head * tokens + y * WIN
                    out_ref[window, start : start + WIN, :] = part + extra


def mean_of(values):
    return jnp.mean(values, axis=-1, keepdims=True)


def norm(values):
    centred = values - mean_of(values)
    scale = lax.rsqrt(mean_of(centred * centred) + NORM_EPS)
    return centred * scale, scale


def norm_back(grad, unit, scale):
    return scale * (grad - mean_of(grad) - unit * mean_of(grad * unit))


def main_kernel(
    heads,
    windows,
    token_ref,
    cot_ref,
    below_ref,
    right_ref,
    diag_ref,
    bias_ref,
    gain1_ref,
    qkv_ref,
    proj_ref,
    gain2_ref,
    fc1_ref,
    fc2_ref,
    own_out,
    below_out,
    right_out,
    diag_out,
    grads_ref,
    x_ref,
    c_ref,
    n_ref,
    unit_ref,
    scale_ref,
    q_ref,
    k_ref,
    v_ref,
    p_ref,
    att_ref,
    dh_ref,
    dqkv_ref,
    ds_ref,
    out_ref,
):
    tokens = WIN * WIN
    width = token_ref.shape[2]
    head_size = width // heads
    total = windows * tokens
    hidden_units = fc1_ref.shape[1]

    def assemble(tile_ref, index, target):
        tile = tile_ref[...].astype(F32)
        below = below_ref[index].astype(F32)
        right = right_ref[index].astype(F32)
        diag = diag_ref[index].astype(F32)
        for window in range(windows):
            start = WIN * window
            if window < windows - 1:
                top = tile[SHIFT:, start + SHIFT : start + SHIFT + WIN]
                low = below[:, start : start + WIN]
            else:
                top = jnp.concatenate([tile[SHIFT:, start + SHIFT :], right], 1)
                low = jnp.concatenate([below[:, start:], diag], 1)
            both = jnp.concatenate([top, low], 0).reshape(tokens, width)
            target[window * tokens : (window + 1) * tokens, :] = both.astype(target.dtype)

    assemble(token_ref, 0, x_ref)
    assemble(cot_ref, 1, c_ref)

    unit1, scale1 = norm(x_ref[...])
    unit_ref[...] = unit1
    scale_ref[...] = scale1
    normed = (unit1 * gain1_ref[...]).astype(BF16)
    n_ref[...] = normed
    projected = dot(normed, qkv_ref[...], 1, 0)
    q_ref[...] = projected[:, :width]
    k_ref[...] = projected[:, width : 2 * width].astype(BF16)
    v_ref[...] = projected[:, 2 * width :].astype(BF16)
    lane_head = iota((1, width), 1) // head_size
    score_scale = head_size ** (-0.5)

    def of_head(values, head):
        return jnp.where(lane_head == head, values, 0.0).astype(BF16)

    for window in range(windows):
        span = slice(window * tokens, (window + 1) * tokens)
        query = q_ref[span, :]
        keys = k_ref[span, :]
        value = v_ref[span, :].astype(F32)
        attended = jnp.zeros((tokens, width), F32)
        for head in range(heads):
            scores = dot(of_head(query, head), keys, 1, 1) * score_scale
            scores = scores + bias_ref[window, head * tokens : (head + 1) * tokens, :]
            shifted = scores - jnp.max(scores, axis=-1, keepdims=True)
            exponent = jnp.exp(shifted)
            inverse = 1.0 / jnp.sum(exponent, axis=-1, keepdims=True)
            weights = (exponent * inverse).astype(BF16)
            p_ref[window * heads + head] = weights
            attended = attended + dot(weights, of_head(value, head), 1, 0)
        att_ref[span, :] = attended.astype(BF16)

    hidden = x_ref[...] + dot(att_ref[...], proj_ref[...], 1, 0).astype(BF16).astype(F32)
    unit2, scale2 = norm(hidden)
    normed2 = (unit2 * gain2_ref[...]).astype(BF16)
    cot = c_ref[...]
    moved = hidden
    back = jnp.zeros((total, width), F32)
    root = math.sqrt(0.5)
    for part in range(hidden_units // width):
        cols = slice(part * width, (part + 1) * width)
        before = dot(normed2, fc1_ref[:, cols], 1, 0)
        normal = 0.5 * (1.0 + lax.erf(before * root))
        inner = (before * normal).astype(BF16)
        slope = normal + before * (jnp.exp(-0.5 * before * before) * (1.0 / math.sqrt(2.0 * math.pi)))
        grad_inner = dot(cot, fc2_ref[cols, :], 1, 1).astype(BF16).astype(F32)
        grad_before = (grad_inner * slope).astype(BF16)
        moved = moved + dot(inner, fc2_ref[cols, :], 1, 0)
        back = back + dot(grad_before, fc1_ref[:, cols], 1, 1)
        grads_ref[part * width : (part + 1) * width, :] = dot(normed2, grad_before, 0, 0).astype(BF16)
        start = hidden_units + part * width
        grads_ref[start : start + width, :] = dot(inner, cot, 0, 0).astype(BF16)
    out_ref[...] = moved
    back = back.astype(BF16).astype(F32)
    grad_gain2 = jnp.sum(back * unit2, axis=0, keepdims=True)
    grad_hidden = cot.astype(F32) + norm_back(back * gain2_ref[...], unit2, scale2)
    dh_ref[...] = grad_hidden

    grad_attended = grad_hidden.astype(BF16)
    row = 2 * hidden_units + 3 * width
    grads_ref[row : row + width, :] = dot(att_ref[...], grad_attended, 0, 0).astype(BF16)
    grad_heads = dot(grad_attended, proj_ref[...], 1, 1).astype(BF16).astype(F32)

    for window in range(windows):
        span = slice(window * tokens, (window + 1) * tokens)
        query = q_ref[span, :]
        keys = k_ref[span, :].astype(F32)
        value = v_ref[span, :]
        grad_out = grad_heads[span, :]
        grad_q = jnp.zeros((tokens, width), F32)
        grad_k = jnp.zeros((tokens, width), F32)
        grad_v = jnp.zeros((tokens, width), F32)
        for head in range(heads):
            grad_part = of_head(grad_out, head)
            weights = p_ref[window * heads + head]
            grad_weights = dot(grad_part, value, 1, 1)
            product = grad_weights * weights.astype(F32)
            inside = jnp.sum(product, axis=-1, keepdims=True)
            grad_scores = product - weights.astype(F32) * inside
            rows = slice(head * tokens, (head + 1) * tokens)
            if window == 0:
                ds_ref[rows, :] = grad_scores
            else:
                ds_ref[rows, :] += grad_scores
            narrow = grad_scores.astype(BF16)
            grad_q = grad_q + dot(narrow, of_head(keys, head), 1, 0)
            grad_k = grad_k + dot(narrow, of_head(query, head), 0, 0)
            grad_v = grad_v + dot(weights, grad_part, 0, 0)
        dqkv_ref[span, :width] = (grad_q * score_scale).astype(BF16)
        dqkv_ref[span, width : 2 * width] = (grad_k * score_scale).astype(BF16)
        dqkv_ref[span, 2 * width :] = grad_v.astype(BF16)

    grad_projected = dqkv_ref[...]
    grad_qkv = dot(n_ref[...], grad_projected, 0, 0).astype(BF16)
    for part in range(3):
        row = 2 * hidden_units + part * width
        grads_ref[row : row + width, :] = grad_qkv[:, part * width : (part + 1) * width]
    grad_normed = dot(grad_projected, qkv_ref[...], 1, 1).astype(BF16).astype(F32)
    unit1 = unit_ref[...]
    grad_gain1 = jnp.sum(grad_normed * unit1, axis=0, keepdims=True)
    grad_x = dh_ref[...] + norm_back(grad_normed * gain1_ref[...], unit1, scale_ref[...])

    lanes = 2 * tokens
    rows = heads * WIN
    blank = jnp.zeros((WIN, LANES), F32)
    strip = jnp.zeros((rows, lanes), F32)
    for fine in range(8):
        near, far = WIN - 1 - fine, WIN - 9 - fine
        blocks = []
        for head in range(heads):
            first = ds_ref[head * tokens + near * WIN : head * tokens + (near + 1) * WIN, :]
            second = ds_ref[head * tokens + far * WIN : head * tokens + (far + 1) * WIN, :]
            blocks.append(
                jnp.concatenate([first, blank, blank], 1)
                + jnp.concatenate([blank, second, blank], 1)
            )
        block = jnp.concatenate(blocks, 0)
        strip = strip + (pltpu.roll(block, WIN * fine, 1) if fine else block)
    lane = iota((rows, lanes), 1)
    amounts = WIN - 1 - iota((rows, lanes), 0) % WIN
    offsets = 2 * WIN
    table = jnp.zeros((2 * heads * offsets, LANES), F32)
    for odd in range(2):
        chosen = jnp.where((lane // WIN) % 2 == odd, strip, 0.0)
        if odd:
            chosen = pltpu.roll(chosen, lanes - WIN, 1)
        chosen = shift_rows(chosen, amounts, True)
        where_row = (iota((offsets, lanes), 1) // 32) * 2 + odd == offsets - 2 - iota((offsets, lanes), 0)
        terms = []
        for head in range(heads):
            flat = jnp.sum(chosen[head * WIN : (head + 1) * WIN, :], axis=0, keepdims=True)
            terms.append(jnp.where(where_row, flat, 0.0))
        terms = jnp.concatenate(terms, 0)
        high = terms.astype(BF16)
        low = (terms - high.astype(F32)).astype(BF16)
        pick_lane = iota((lanes, LANES), 0) % 32
        pick = jnp.where(pick_lane == offsets - 2 - iota((lanes, LANES), 1), 1.0, 0.0).astype(BF16)
        table = table + dot(jnp.concatenate([high, low], 0), pick, 1, 0)
    table = table[: heads * offsets] + table[heads * offsets :]
    row = 2 * hidden_units + 4 * width
    grads_ref[row : row + heads * offsets, :] = table.astype(BF16)
    row = row + heads * offsets
    rest = jnp.concatenate(
        [grad_gain1, grad_gain2, jnp.zeros((grads_ref.shape[0] - row - 2, width), F32)], 0
    )
    grads_ref[row:, :] = rest.astype(BF16)

    def scatter(values, index):
        for window in range(windows):
            start = WIN * window
            block = values[window * tokens : (window + 1) * tokens, :].reshape(WIN, WIN, width)
            block = block.astype(F32)
            top, low = block[:SHIFT], block[SHIFT:]
            if window < windows - 1:
                own_out[index, :, start : start + WIN, :] = top.astype(BF16)
                below_out[index, :, start : start + WIN, :] = low.astype(BF16)
            else:
                own_out[index, :, start:, :] = top[:, :SHIFT].astype(BF16)
                below_out[index, :, start:, :] = low[:, :SHIFT].astype(BF16)
                right_out[index] = top[:, SHIFT:].astype(BF16)
                diag_out[index] = low[:, SHIFT:].astype(BF16)

    scatter(out_ref[...], 0)
    scatter(grad_x, 1)


def sum_kernel(in_ref, out_ref):
    total = in_ref[0].astype(F32)
    for index in range(1, in_ref.shape[0]):
        total = total + in_ref[index].astype(F32)
    out_ref[...] = total.astype(out_ref.dtype)


def unpack_kernel(
    heads,
    factor,
    summed_ref,
    gain1_ref,
    qkv_ref,
    proj_ref,
    table_ref,
    gain2_ref,
    fc1_ref,
    fc2_ref,
):
    width, hidden_units = fc1_ref.shape
    offsets = 2 * WIN

    def rows(start, count):
        return summed_ref[start : start + count, :].astype(F32) * factor

    for part in range(hidden_units // width):
        fc1_ref[:, part * width : (part + 1) * width] = rows(part * width, width)
    fc2_ref[...] = rows(hidden_units, hidden_units)
    for part in range(3):
        qkv_ref[:, part * width : (part + 1) * width] = rows(2 * hidden_units + part * width, width)
    start = 2 * hidden_units + 3 * width
    proj_ref[...] = rows(start, width)
    start = start + width
    for head in range(heads):
        block = rows(start + head * offsets, offsets)
        table_ref[head] = block[: offsets - 1, : offsets - 1]
    start = start + heads * offsets
    gains = rows(start, 16)
    gain1_ref[...] = gains[0:1]
    gain2_ref[...] = gains[1:2]


def neighbour_pairs(row_step, col_step):
    groups, tiles = lax.axis_size("group"), lax.axis_size("tile")
    pairs = []
    for group in range(groups):
        for tile in range(tiles):
            target = ((group + row_step) % groups) * tiles + (tile + col_step) % tiles
            pairs.append((group * tiles + tile, target))
    return pairs


def passed_along(value, row_step, col_step):
    return lax.ppermute(value, AXES, neighbour_pairs(row_step, col_step))


def shards(tokens, gain1, w_qkv, w_proj, bias_table, gain2, w_fc1, w_fc2, cotangent):
    row_count, col_count, width = tokens.shape
    heads = bias_table.shape[0]
    hidden_units = w_fc1.shape[1]
    groups, tiles = lax.axis_size("group"), lax.axis_size("tile")
    devices = groups * tiles
    windows = col_count // WIN
    token_count = WIN * WIN
    total = windows * token_count
    keep = col_count - SHIFT

    both = jnp.stack([tokens, cotangent])
    below = passed_along(both[:, :SHIFT, SHIFT:], -1, 0)
    right = passed_along(both[:, SHIFT:, :SHIFT], 0, -1)
    diag = passed_along(both[:, :SHIFT, :SHIFT], -1, -1)

    flags = jnp.stack(
        [
            (lax.axis_index("group") == groups - 1).astype(jnp.int32),
            (lax.axis_index("tile") == tiles - 1).astype(jnp.int32),
        ]
    )
    vmem = pl.BlockSpec(memory_space=pltpu.VMEM)
    smem = pl.BlockSpec(memory_space=pltpu.SMEM)
    bias = pl.pallas_call(
        functools.partial(bias_kernel, heads, windows),
        out_shape=jax.ShapeDtypeStruct((windows, heads * token_count, token_count), F32),
        in_specs=[smem, vmem],
        out_specs=vmem,
        name="bias",
        cost_estimate=pl.CostEstimate(flops=8_000_000, bytes_accessed=2_000_000, transcendentals=0),
    )(flags, bias_table)

    used = 2 * hidden_units + 4 * width + heads * 2 * WIN + 16
    chunk = (used + devices * 8 - 1) // (devices * 8) * 8
    grad_rows = chunk * devices
    own_out, below_out, right_out, diag_out, grads = pl.pallas_call(
        functools.partial(main_kernel, heads, windows),
        out_shape=(
            jax.ShapeDtypeStruct((2, SHIFT, keep, width), BF16),
            jax.ShapeDtypeStruct((2, SHIFT, keep, width), BF16),
            jax.ShapeDtypeStruct((2, SHIFT, SHIFT, width), BF16),
            jax.ShapeDtypeStruct((2, SHIFT, SHIFT, width), BF16),
            jax.ShapeDtypeStruct((grad_rows, width), BF16),
        ),
        in_specs=[vmem] * 12,
        out_specs=(vmem,) * 5,
        scratch_shapes=[
            pltpu.VMEM((total, width), F32),
            pltpu.VMEM((total, width), BF16),
            pltpu.VMEM((total, width), BF16),
            pltpu.VMEM((total, width), F32),
            pltpu.VMEM((total, 1), F32),
            pltpu.VMEM((total, width), F32),
            pltpu.VMEM((total, width), BF16),
            pltpu.VMEM((total, width), BF16),
            pltpu.VMEM((windows * heads, token_count, token_count), BF16),
            pltpu.VMEM((total, width), BF16),
            pltpu.VMEM((total, width), F32),
            pltpu.VMEM((total, 3 * width), BF16),
            pltpu.VMEM((heads * token_count, token_count), F32),
            pltpu.VMEM((total, width), F32),
        ],
        name="block",
        cost_estimate=pl.CostEstimate(
            flops=2_000_000_000, bytes_accessed=4_000_000, transcendentals=2_000_000
        ),
    )(
        tokens,
        cotangent,
        below,
        right,
        diag,
        bias,
        gain1.reshape(1, width),
        w_qkv,
        w_proj,
        gain2.reshape(1, width),
        w_fc1,
        w_fc2,
    )

    back_below = passed_along(below_out, 1, 0)
    back_right = passed_along(right_out, 0, 1)
    back_diag = passed_along(diag_out, 1, 1)

    spread = lax.all_to_all(grads.reshape(devices, chunk, width), AXES, 0, 0, tiled=True)
    partial = pl.pallas_call(
        sum_kernel,
        out_shape=jax.ShapeDtypeStruct((chunk, width), BF16),
        in_specs=[vmem],
        out_specs=vmem,
        name="add",
    )(spread)
    copies = jnp.broadcast_to(partial[None], (devices, chunk, width))
    summed = lax.all_to_all(copies, AXES, 0, 0, tiled=True).reshape(grad_rows, width)

    factor = 1.0 / math.sqrt(row_count * groups * col_count * tiles)
    grad_gain1, grad_qkv, grad_proj, grad_table, grad_gain2, grad_fc1, grad_fc2 = pl.pallas_call(
        functools.partial(unpack_kernel, heads, factor),
        out_shape=(
            jax.ShapeDtypeStruct((1, width), F32),
            jax.ShapeDtypeStruct(w_qkv.shape, F32),
            jax.ShapeDtypeStruct(w_proj.shape, F32),
            jax.ShapeDtypeStruct(bias_table.shape, F32),
            jax.ShapeDtypeStruct((1, width), F32),
            jax.ShapeDtypeStruct(w_fc1.shape, F32),
            jax.ShapeDtypeStruct(w_fc2.shape, F32),
        ),
        in_specs=[vmem],
        out_specs=(vmem,) * 7,
        name="unpack",
    )(summed)

    high = jnp.concatenate([back_diag, back_below], 2)
    low = jnp.concatenate([back_right, own_out], 2)
    whole = jnp.concatenate([high, low], 1)
    return (
        whole[0],
        whole[1],
        grad_gain1.reshape(width),
        grad_qkv,
        grad_proj,
        grad_table,
        grad_gain2.reshape(width),
        grad_fc1,
        grad_fc2,
    )


def solution(mesh):
    tile_spec = P("group", "tile", None)
    return jax.shard_map(
        shards,
        mesh=mesh,
        in_specs=(tile_spec, P(), P(), P(), P(), P(), P(), P(), tile_spec),
        out_specs=(tile_spec, tile_spec, P(), P(), P(), P(), P(), P(), P()),
        check_vma=False,
    )
```

```python
import functools
import math

import jax
import jax.numpy as jnp
from jax import lax
from jax.experimental import pallas as pl
from jax.experimental.pallas import tpu as pltpu
from jax.sharding import PartitionSpec as P

WIN = 16
SHIFT = 8
NORM_EPS = 1e-05
LANES = 128
F32 = jnp.float32
BF16 = jnp.bfloat16
AXES = ("group", "tile")
PARAMS = pltpu.CompilerParams(vmem_limit_bytes=24 * 1024 * 1024)


def dot(left, right, left_dim, right_dim, precision=None):
    return lax.dot_general(
        left,
        right,
        (((left_dim,), (right_dim,)), ((), ())),
        preferred_element_type=F32,
        precision=precision,
    )


def iota(shape, dim):
    return lax.broadcasted_iota(jnp.int32, shape, dim)


def shift_rows(values, amounts, right):
    width = values.shape[1]
    for bit in range(4):
        step = 1 << bit
        moved = pltpu.roll(values, step if right else width - step, 1)
        values = jnp.where((amounts & step) != 0, moved, values)
    return values


def bias_kernel(heads, windows, table_ref, out_ref):
    span = 2 * WIN * WIN
    tokens = WIN * WIN
    offsets = 2 * WIN - 1
    lane = iota((offsets, span), 1)
    row = iota((offsets, span), 0)
    flats = []
    for odd in range(2):
        pick = jnp.where(lane % 32 == offsets - 1 - row, 1.0, 0.0).astype(F32)
        keep = (lane // 32) * 2 + odd == offsets - 1 - row
        for head in range(heads):
            spread = dot(table_ref[:, head, :], pick, 1, 0, lax.Precision.HIGHEST)
            flat = jnp.sum(jnp.where(keep, spread, 0.0), axis=0, keepdims=True)
            flats.append(jnp.broadcast_to(flat, (WIN, span)))
    rows = heads * WIN
    amounts = WIN - 1 - iota((rows, span), 0) % WIN
    even = shift_rows(jnp.concatenate(flats[:heads], 0), amounts, False)
    odd = shift_rows(jnp.concatenate(flats[heads:], 0), amounts, False)
    odd = pltpu.roll(odd, WIN, 1)
    strip = jnp.where(iota((rows, span), 1) % 32 < WIN, even, odd)
    last_row = (lax.axis_index("group") == lax.axis_size("group") - 1).astype(jnp.int32)
    last_col = (lax.axis_index("tile") == lax.axis_size("tile") - 1).astype(jnp.int32)
    key = iota((WIN, tokens), 1)
    query_x = iota((WIN, tokens), 0)
    key_low = (key >= tokens // 2).astype(jnp.int32)
    cross_col = ((key % WIN >= SHIFT) != (query_x >= SHIFT)).astype(jnp.int32)
    for fine in range(8):
        moved = pltpu.roll(strip, (span - WIN * fine) % span, 1)
        for coarse in range(2):
            y = WIN - 1 - (8 * coarse + fine)
            cross_row = key_low if y < SHIFT else 1 - key_low
            for window in range(windows):
                apart = cross_row * last_row
                if window == windows - 1:
                    apart = apart + cross_col * last_col
                extra = jnp.where(apart > 0, -1e30, 0.0)
                for head in range(heads):
                    part = moved[
                        head * WIN : (head + 1) * WIN,
                        LANES * coarse : LANES * coarse + tokens,
                    ]
                    start = head * tokens + y * WIN
                    out_ref[window, start : start + WIN, :] = part + extra


def mean_of(values):
    return jnp.mean(values, axis=-1, keepdims=True)


def norm(values):
    centred = values - mean_of(values)
    scale = lax.rsqrt(mean_of(centred * centred) + NORM_EPS)
    return centred * scale, scale


def norm_back(grad, unit, scale):
    return scale * (grad - mean_of(grad) - unit * mean_of(grad * unit))


def main_kernel(
    heads,
    windows,
    token_ref,
    cot_ref,
    below_ref,
    right_ref,
    diag_ref,
    bias_ref,
    gain1_ref,
    qkv_ref,
    proj_ref,
    gain2_ref,
    fc1_ref,
    fc2_ref,
    own_out,
    below_out,
    right_out,
    diag_out,
    keep_out,
    send_out,
    grads_ref,
    x_ref,
    c_ref,
    n_ref,
    unit_ref,
    scale_ref,
    q_ref,
    k_ref,
    v_ref,
    p_ref,
    att_ref,
    dh_ref,
    dqkv_ref,
    ds_ref,
    out_ref,
):
    tokens = WIN * WIN
    width = token_ref.shape[2]
    head_size = width // heads
    total = windows * tokens
    hidden_units = fc1_ref.shape[1]

    def assemble(tile_ref, index, target):
        tile = tile_ref[...].astype(F32)
        below = below_ref[index].astype(F32)
        right = right_ref[index].astype(F32)
        diag = diag_ref[index].astype(F32)
        for window in range(windows):
            start = WIN * window
            if window < windows - 1:
                top = tile[SHIFT:, start + SHIFT : start + SHIFT + WIN]
                low = below[:, start : start + WIN]
            else:
                top = jnp.concatenate([tile[SHIFT:, start + SHIFT :], right], 1)
                low = jnp.concatenate([below[:, start:], diag], 1)
            both = jnp.concatenate([top, low], 0).reshape(tokens, width)
            target[window * tokens : (window + 1) * tokens, :] = both.astype(target.dtype)

    assemble(token_ref, 0, x_ref)
    assemble(cot_ref, 1, c_ref)

    unit1, scale1 = norm(x_ref[...])
    unit_ref[...] = unit1
    scale_ref[...] = scale1
    normed = (unit1 * gain1_ref[...]).astype(BF16)
    n_ref[...] = normed
    projected = dot(normed, qkv_ref[...], 1, 0)
    q_ref[...] = projected[:, :width]
    k_ref[...] = projected[:, width : 2 * width].astype(BF16)
    v_ref[...] = projected[:, 2 * width :].astype(BF16)
    lane_head = iota((1, width), 1) // head_size
    score_scale = head_size ** (-0.5)

    def of_head(values, head):
        return jnp.where(lane_head == head, values, 0.0).astype(BF16)

    for window in range(windows):
        span = slice(window * tokens, (window + 1) * tokens)
        query = q_ref[span, :]
        keys = k_ref[span, :]
        value = v_ref[span, :].astype(F32)
        attended = jnp.zeros((tokens, width), F32)
        for head in range(heads):
            scores = dot(of_head(query, head), keys, 1, 1) * score_scale
            scores = scores + bias_ref[window, head * tokens : (head + 1) * tokens, :]
            shifted = scores - jnp.max(scores, axis=-1, keepdims=True)
            exponent = jnp.exp(shifted)
            inverse = 1.0 / jnp.sum(exponent, axis=-1, keepdims=True)
            weights = (exponent * inverse).astype(BF16)
            p_ref[window * heads + head] = weights
            attended = attended + dot(weights, of_head(value, head), 1, 0)
        att_ref[span, :] = attended.astype(BF16)

    hidden = x_ref[...] + dot(att_ref[...], proj_ref[...], 1, 0).astype(BF16).astype(F32)
    unit2, scale2 = norm(hidden)
    normed2 = (unit2 * gain2_ref[...]).astype(BF16)
    cot = c_ref[...]
    moved = hidden
    back = jnp.zeros((total, width), F32)
    root = math.sqrt(0.5)
    for part in range(hidden_units // width):
        cols = slice(part * width, (part + 1) * width)
        before = dot(normed2, fc1_ref[:, cols], 1, 0)
        normal = 0.5 * (1.0 + lax.erf(before * root))
        inner = (before * normal).astype(BF16)
        slope = normal + before * (jnp.exp(-0.5 * before * before) * (1.0 / math.sqrt(2.0 * math.pi)))
        grad_inner = dot(cot, fc2_ref[cols, :], 1, 1).astype(BF16).astype(F32)
        grad_before = (grad_inner * slope).astype(BF16)
        moved = moved + dot(inner, fc2_ref[cols, :], 1, 0)
        back = back + dot(grad_before, fc1_ref[:, cols], 1, 1)
        grads_ref[part * width : (part + 1) * width, :] = dot(normed2, grad_before, 0, 0).astype(BF16)
        start = hidden_units + part * width
        grads_ref[start : start + width, :] = dot(inner, cot, 0, 0).astype(BF16)
    out_ref[...] = moved
    back = back.astype(BF16).astype(F32)
    grad_gain2 = jnp.sum(back * unit2, axis=0, keepdims=True)
    grad_hidden = cot.astype(F32) + norm_back(back * gain2_ref[...], unit2, scale2)
    dh_ref[...] = grad_hidden

    grad_attended = grad_hidden.astype(BF16)
    row = 2 * hidden_units + 3 * width
    grads_ref[row : row + width, :] = dot(att_ref[...], grad_attended, 0, 0).astype(BF16)
    grad_heads = dot(grad_attended, proj_ref[...], 1, 1).astype(BF16).astype(F32)

    for window in range(windows):
        span = slice(window * tokens, (window + 1) * tokens)
        query = q_ref[span, :]
        keys = k_ref[span, :].astype(F32)
        value = v_ref[span, :]
        grad_out = grad_heads[span, :]
        grad_q = jnp.zeros((tokens, width), F32)
        grad_k = jnp.zeros((tokens, width), F32)
        grad_v = jnp.zeros((tokens, width), F32)
        for head in range(heads):
            grad_part = of_head(grad_out, head)
            weights = p_ref[window * heads + head]
            grad_weights = dot(grad_part, value, 1, 1)
            product = grad_weights * weights.astype(F32)
            inside = jnp.sum(product, axis=-1, keepdims=True)
            grad_scores = product - weights.astype(F32) * inside
            rows = slice(head * tokens, (head + 1) * tokens)
            if window == 0:
                ds_ref[rows, :] = grad_scores
            else:
                ds_ref[rows, :] += grad_scores
            narrow = grad_scores.astype(BF16)
            grad_q = grad_q + dot(narrow, of_head(keys, head), 1, 0)
            grad_k = grad_k + dot(narrow, of_head(query, head), 0, 0)
            grad_v = grad_v + dot(weights, grad_part, 0, 0)
        dqkv_ref[span, :width] = (grad_q * score_scale).astype(BF16)
        dqkv_ref[span, width : 2 * width] = (grad_k * score_scale).astype(BF16)
        dqkv_ref[span, 2 * width :] = grad_v.astype(BF16)

    grad_projected = dqkv_ref[...]
    grad_qkv = dot(n_ref[...], grad_projected, 0, 0).astype(BF16)
    for part in range(3):
        row = 2 * hidden_units + part * width
        grads_ref[row : row + width, :] = grad_qkv[:, part * width : (part + 1) * width]
    grad_normed = dot(grad_projected, qkv_ref[...], 1, 1).astype(BF16).astype(F32)
    unit1 = unit_ref[...]
    grad_gain1 = jnp.sum(grad_normed * unit1, axis=0, keepdims=True)
    grad_x = dh_ref[...] + norm_back(grad_normed * gain1_ref[...], unit1, scale_ref[...])

    lanes = 2 * tokens
    rows = heads * WIN
    blank = jnp.zeros((WIN, LANES), F32)
    strip = jnp.zeros((rows, lanes), F32)
    for fine in range(8):
        near, far = WIN - 1 - fine, WIN - 9 - fine
        blocks = []
        for head in range(heads):
            first = ds_ref[head * tokens + near * WIN : head * tokens + (near + 1) * WIN, :]
            second = ds_ref[head * tokens + far * WIN : head * tokens + (far + 1) * WIN, :]
            blocks.append(
                jnp.concatenate([first, blank, blank], 1)
                + jnp.concatenate([blank, second, blank], 1)
            )
        block = jnp.concatenate(blocks, 0)
        strip = strip + (pltpu.roll(block, WIN * fine, 1) if fine else block)
    lane = iota((rows, lanes), 1)
    amounts = WIN - 1 - iota((rows, lanes), 0) % WIN
    offsets = 2 * WIN
    table = jnp.zeros((2 * heads * offsets, LANES), F32)
    for odd in range(2):
        chosen = jnp.where((lane // WIN) % 2 == odd, strip, 0.0)
        if odd:
            chosen = pltpu.roll(chosen, lanes - WIN, 1)
        chosen = shift_rows(chosen, amounts, True)
        where_row = (iota((offsets, lanes), 1) // 32) * 2 + odd == offsets - 2 - iota((offsets, lanes), 0)
        terms = []
        for head in range(heads):
            flat = jnp.sum(chosen[head * WIN : (head + 1) * WIN, :], axis=0, keepdims=True)
            terms.append(jnp.where(where_row, flat, 0.0))
        terms = jnp.concatenate(terms, 0)
        high = terms.astype(BF16)
        low = (terms - high.astype(F32)).astype(BF16)
        pick_lane = iota((lanes, LANES), 0) % 32
        pick = jnp.where(pick_lane == offsets - 2 - iota((lanes, LANES), 1), 1.0, 0.0).astype(BF16)
        table = table + dot(jnp.concatenate([high, low], 0), pick, 1, 0)
    table = table[: heads * offsets] + table[heads * offsets :]
    row = 2 * hidden_units + 4 * width
    grads_ref[row : row + heads * offsets, :] = table.astype(BF16)
    row = row + heads * offsets
    rest = jnp.concatenate(
        [grad_gain1, grad_gain2, jnp.zeros((grads_ref.shape[0] - row - 2, width), F32)], 0
    )
    grads_ref[row:, :] = rest.astype(BF16)
    half = keep_out.shape[0]
    core = lax.axis_index("group") % 2
    keep_out[...] = grads_ref[pl.ds(pl.multiple_of(core * half, 16), half), :]
    send_out[...] = grads_ref[pl.ds(pl.multiple_of((1 - core) * half, 16), half), :]

    def scatter(values, index):
        for window in range(windows):
            start = WIN * window
            block = values[window * tokens : (window + 1) * tokens, :].reshape(WIN, WIN, width)
            block = block.astype(F32)
            top, low = block[:SHIFT], block[SHIFT:]
            if window < windows - 1:
                own_out[index, :, start : start + WIN, :] = top.astype(BF16)
                below_out[index, :, start : start + WIN, :] = low.astype(BF16)
            else:
                own_out[index, :, start:, :] = top[:, :SHIFT].astype(BF16)
                below_out[index, :, start:, :] = low[:, :SHIFT].astype(BF16)
                right_out[index] = top[:, SHIFT:].astype(BF16)
                diag_out[index] = low[:, SHIFT:].astype(BF16)

    scatter(out_ref[...], 0)
    scatter(grad_x, 1)


def pair_kernel(first_ref, second_ref, out_ref):
    total = first_ref[...].astype(F32) + second_ref[...].astype(F32)
    out_ref[...] = total.astype(out_ref.dtype)


def sum_kernel(in_ref, out_ref):
    total = in_ref[0].astype(F32)
    for index in range(1, in_ref.shape[0]):
        total = total + in_ref[index].astype(F32)
    total = total.astype(out_ref.dtype)
    for index in range(out_ref.shape[0]):
        out_ref[index] = total


def unpack_kernel(
    heads,
    factor,
    mine_ref,
    other_ref,
    gain1_ref,
    qkv_ref,
    proj_ref,
    table_ref,
    gain2_ref,
    fc1_ref,
    fc2_ref,
    summed_ref,
):
    width, hidden_units = fc1_ref.shape
    half = mine_ref.shape[0]
    core = lax.axis_index("group") % 2
    summed_ref[pl.ds(pl.multiple_of(core * half, 16), half), :] = mine_ref[...]
    summed_ref[pl.ds(pl.multiple_of((1 - core) * half, 16), half), :] = other_ref[...]
    offsets = 2 * WIN

    def rows(start, count):
        return summed_ref[start : start + count, :].astype(F32) * factor

    for part in range(hidden_units // width):
        fc1_ref[:, part * width : (part + 1) * width] = rows(part * width, width)
    fc2_ref[...] = rows(hidden_units, hidden_units)
    for part in range(3):
        qkv_ref[:, part * width : (part + 1) * width] = rows(2 * hidden_units + part * width, width)
    start = 2 * hidden_units + 3 * width
    proj_ref[...] = rows(start, width)
    start = start + width
    for head in range(heads):
        block = rows(start + head * offsets, offsets)
        table_ref[:, head, :] = block[: offsets - 1, : offsets - 1]
    start = start + heads * offsets
    gains = rows(start, 16)
    gain1_ref[...] = gains[0:1]
    gain2_ref[...] = gains[1:2]


def neighbour_pairs(row_step, col_step):
    groups, tiles = lax.axis_size("group"), lax.axis_size("tile")
    pairs = []
    for group in range(groups):
        for tile in range(tiles):
            target = ((group + row_step) % groups) * tiles + (tile + col_step) % tiles
            pairs.append((group * tiles + tile, target))
    return pairs


def passed_along(value, row_step, col_step):
    return lax.ppermute(value, AXES, neighbour_pairs(row_step, col_step))


def shards(tokens, gain1, w_qkv, w_proj, bias_table, gain2, w_fc1, w_fc2, cotangent):
    row_count, col_count, width = tokens.shape
    heads = bias_table.shape[0]
    hidden_units = w_fc1.shape[1]
    groups, tiles = lax.axis_size("group"), lax.axis_size("tile")
    devices = groups * tiles
    windows = col_count // WIN
    token_count = WIN * WIN
    total = windows * token_count
    keep = col_count - SHIFT

    both = jnp.stack([tokens, cotangent])
    below = passed_along(both[:, :SHIFT, SHIFT:], -1, 0)
    right = passed_along(both[:, SHIFT:, :SHIFT], 0, -1)
    diag = passed_along(both[:, :SHIFT, :SHIFT], -1, -1)

    vmem = pl.BlockSpec(memory_space=pltpu.VMEM)
    bias = pl.pallas_call(
        functools.partial(bias_kernel, heads, windows),
        out_shape=jax.ShapeDtypeStruct((windows, heads * token_count, token_count), F32),
        in_specs=[vmem],
        out_specs=vmem,
        name="bias",
        compiler_params=PARAMS,
        cost_estimate=pl.CostEstimate(flops=8_000_000, bytes_accessed=2_000_000, transcendentals=0),
    )(bias_table.transpose(1, 0, 2))

    used = 2 * hidden_units + 4 * width + heads * 2 * WIN + 16
    members = devices // 2
    chunk = (used + devices * 8 - 1) // (devices * 8) * 8
    half = chunk * members
    own_out, below_out, right_out, diag_out, kept, sent = pl.pallas_call(
        functools.partial(main_kernel, heads, windows),
        out_shape=(
            jax.ShapeDtypeStruct((2, SHIFT, keep, width), BF16),
            jax.ShapeDtypeStruct((2, SHIFT, keep, width), BF16),
            jax.ShapeDtypeStruct((2, SHIFT, SHIFT, width), BF16),
            jax.ShapeDtypeStruct((2, SHIFT, SHIFT, width), BF16),
            jax.ShapeDtypeStruct((half, width), BF16),
            jax.ShapeDtypeStruct((half, width), BF16),
        ),
        in_specs=[vmem] * 12,
        out_specs=(vmem,) * 6,
        scratch_shapes=[
            pltpu.VMEM((2 * half, width), BF16),
            pltpu.VMEM((total, width), F32),
            pltpu.VMEM((total, width), BF16),
            pltpu.VMEM((total, width), BF16),
            pltpu.VMEM((total, width), F32),
            pltpu.VMEM((total, 1), F32),
            pltpu.VMEM((total, width), F32),
            pltpu.VMEM((total, width), BF16),
            pltpu.VMEM((total, width), BF16),
            pltpu.VMEM((windows * heads, token_count, token_count), BF16),
            pltpu.VMEM((total, width), BF16),
            pltpu.VMEM((total, width), F32),
            pltpu.VMEM((total, 3 * width), BF16),
            pltpu.VMEM((heads * token_count, token_count), F32),
            pltpu.VMEM((total, width), F32),
        ],
        name="block",
        compiler_params=PARAMS,
        cost_estimate=pl.CostEstimate(
            flops=2_000_000_000, bytes_accessed=4_000_000, transcendentals=2_000_000
        ),
    )(
        tokens,
        cotangent,
        below,
        right,
        diag,
        bias,
        gain1.reshape(1, width),
        w_qkv,
        w_proj,
        gain2.reshape(1, width),
        w_fc1,
        w_fc2,
    )

    back_below = passed_along(below_out, 1, 0)
    back_right = passed_along(right_out, 0, 1)
    back_diag = passed_along(diag_out, 1, 1)

    pairs = [(index, index + tiles if index // tiles % 2 == 0 else index - tiles) for index in range(devices)]
    same_core = [
        [index for index in range(devices) if index // tiles % 2 == core] for core in range(2)
    ]

    def exchanged(value):
        return lax.all_to_all(value, AXES, 0, 0, tiled=True, axis_index_groups=same_core)

    received = lax.ppermute(sent, AXES, pairs)
    paired = pl.pallas_call(
        pair_kernel,
        out_shape=jax.ShapeDtypeStruct((half, width), BF16),
        in_specs=[vmem] * 2,
        out_specs=vmem,
        name="pair",
        compiler_params=PARAMS,
    )(kept, received)
    copies = pl.pallas_call(
        sum_kernel,
        out_shape=jax.ShapeDtypeStruct((members, chunk, width), BF16),
        in_specs=[vmem],
        out_specs=vmem,
        name="add",
        compiler_params=PARAMS,
    )(exchanged(paired.reshape(members, chunk, width)))
    mine = exchanged(copies).reshape(half, width)
    other = lax.ppermute(mine, AXES, pairs)

    factor = 1.0 / math.sqrt(row_count * groups * col_count * tiles)
    grad_gain1, grad_qkv, grad_proj, grad_table, grad_gain2, grad_fc1, grad_fc2 = pl.pallas_call(
        functools.partial(unpack_kernel, heads, factor),
        out_shape=(
            jax.ShapeDtypeStruct((1, width), F32),
            jax.ShapeDtypeStruct(w_qkv.shape, F32),
            jax.ShapeDtypeStruct(w_proj.shape, F32),
            jax.ShapeDtypeStruct((bias_table.shape[1], heads, bias_table.shape[2]), F32),
            jax.ShapeDtypeStruct((1, width), F32),
            jax.ShapeDtypeStruct(w_fc1.shape, F32),
            jax.ShapeDtypeStruct(w_fc2.shape, F32),
        ),
        in_specs=[vmem] * 2,
        out_specs=(vmem,) * 7,
        scratch_shapes=[pltpu.VMEM((2 * half, width), BF16)],
        name="unpack",
        compiler_params=PARAMS,
    )(mine, other)

    high = jnp.concatenate([back_diag, back_below], 2)
    low = jnp.concatenate([back_right, own_out], 2)
    whole = jnp.concatenate([high, low], 1)
    return (
        whole[0],
        whole[1],
        grad_gain1.reshape(width),
        grad_qkv,
        grad_proj,
        grad_table.transpose(1, 0, 2),
        grad_gain2.reshape(width),
        grad_fc1,
        grad_fc2,
    )


def solution(mesh):
    tile_spec = P("group", "tile", None)
    return jax.shard_map(
        shards,
        mesh=mesh,
        in_specs=(tile_spec, P(), P(), P(), P(), P(), P(), P(), tile_spec),
        out_specs=(tile_spec, tile_spec, P(), P(), P(), P(), P(), P(), P()),
        check_vma=False,
    )
```

```python
import functools
import math

import jax
import jax.numpy as jnp
from jax import lax
from jax.experimental import pallas as pl
from jax.experimental.pallas import tpu as pltpu
from jax.sharding import PartitionSpec as P

WIN = 16
SHIFT = 8
NORM_EPS = 1e-05
LOG2_E = math.log2(math.e)
LANES = 128
F32 = jnp.float32
BF16 = jnp.bfloat16
AXES = ("group", "tile")
PARAMS = pltpu.CompilerParams(vmem_limit_bytes=24 * 1024 * 1024)


def dot(left, right, left_dim, right_dim, precision=None):
    return lax.dot_general(
        left,
        right,
        (((left_dim,), (right_dim,)), ((), ())),
        preferred_element_type=F32,
        precision=precision,
    )


def iota(shape, dim):
    return lax.broadcasted_iota(jnp.int32, shape, dim)


def shift_rows(values, amounts, right):
    width = values.shape[1]
    for bit in range(4):
        step = 1 << bit
        moved = pltpu.roll(values, step if right else width - step, 1)
        values = jnp.where((amounts & step) != 0, moved, values)
    return values


def bias_kernel(heads, windows, table_ref, out_ref):
    span = 2 * WIN * WIN
    tokens = WIN * WIN
    offsets = 2 * WIN - 1
    lane = iota((offsets, span), 1)
    row = iota((offsets, span), 0)
    flats = []
    for odd in range(2):
        pick = jnp.where(lane % 32 == offsets - 1 - row, 1.0, 0.0).astype(F32)
        keep = (lane // 32) * 2 + odd == offsets - 1 - row
        for head in range(heads):
            spread = dot(table_ref[:, head, :], pick, 1, 0, lax.Precision.HIGHEST)
            flat = jnp.sum(jnp.where(keep, spread, 0.0), axis=0, keepdims=True)
            flats.append(jnp.broadcast_to(flat, (WIN, span)))
    rows = heads * WIN
    amounts = WIN - 1 - iota((rows, span), 0) % WIN
    even = shift_rows(jnp.concatenate(flats[:heads], 0), amounts, False)
    odd = shift_rows(jnp.concatenate(flats[heads:], 0), amounts, False)
    odd = pltpu.roll(odd, WIN, 1)
    strip = jnp.where(iota((rows, span), 1) % 32 < WIN, even, odd) * LOG2_E
    last_row = (lax.axis_index("group") == lax.axis_size("group") - 1).astype(jnp.int32)
    last_col = (lax.axis_index("tile") == lax.axis_size("tile") - 1).astype(jnp.int32)
    key = iota((WIN, tokens), 1)
    query_x = iota((WIN, tokens), 0)
    key_low = (key >= tokens // 2).astype(jnp.int32)
    cross_col = ((key % WIN >= SHIFT) != (query_x >= SHIFT)).astype(jnp.int32)
    for fine in range(8):
        moved = pltpu.roll(strip, (span - WIN * fine) % span, 1)
        for coarse in range(2):
            y = WIN - 1 - (8 * coarse + fine)
            cross_row = key_low if y < SHIFT else 1 - key_low
            for window in range(windows):
                apart = cross_row * last_row
                if window == windows - 1:
                    apart = apart + cross_col * last_col
                extra = jnp.where(apart > 0, -1e30, 0.0)
                for head in range(heads):
                    part = moved[
                        head * WIN : (head + 1) * WIN,
                        LANES * coarse : LANES * coarse + tokens,
                    ]
                    start = head * tokens + y * WIN
                    out_ref[window, start : start + WIN, :] = part + extra


def mean_of(values):
    return jnp.mean(values, axis=-1, keepdims=True)


def norm(values):
    centred = values - mean_of(values)
    scale = lax.rsqrt(mean_of(centred * centred) + NORM_EPS)
    return centred * scale, scale


def norm_back(grad, unit, scale):
    return scale * (grad - mean_of(grad) - unit * mean_of(grad * unit))


def cut_kernel(token_ref, cot_ref, below_ref, right_ref, diag_ref):
    for index, tile_ref in enumerate((token_ref, cot_ref)):
        below_ref[index] = tile_ref[:SHIFT, SHIFT:, :]
        right_ref[index] = tile_ref[SHIFT:, :SHIFT, :]
        diag_ref[index] = tile_ref[:SHIFT, :SHIFT, :]


def block_kernel(heads, first, count, last, *refs):
    token_ref, cot_ref, below_ref = refs[:3]
    refs = refs[3:]
    if last:
        right_ref, diag_ref, sums_in, strip_in, gains_in = refs[:5]
        refs = refs[5:]
    bias_ref, gain1_ref, qkv_ref, proj_ref, gain2_ref, fc1_ref, fc2_ref = refs[:7]
    own_out, below_out = refs[7:9]
    refs = refs[9:]
    if last:
        right_out, diag_out, keep_out, send_out, grads_ref = refs[:5]
        refs = refs[5:]
    else:
        sums_out, strip_out, gains_out = refs[:3]
        refs = refs[3:]
    x_ref, c_ref, n_ref, unit_ref, scale_ref, q_ref, k_ref, v_ref = refs[:8]
    p_ref, att_ref, out_f32_ref, inverse_ref, dh_ref, dqkv_ref, ds_ref, dsn_ref = refs[8:16]
    inner_ref, before_ref, out_ref = refs[16:]

    tokens = WIN * WIN
    width = token_ref.shape[2]
    head_size = width // heads
    total = count * tokens
    hidden_units = fc1_ref.shape[1]

    def put(row, value):
        rows = slice(row, row + value.shape[0])
        if last:
            grads_ref[rows, :] = (sums_in[rows, :] + value).astype(BF16)
        else:
            sums_out[rows, :] = value

    def assemble(tile_ref, index, target):
        tile = tile_ref[...].astype(F32)
        below = below_ref[index].astype(F32)
        for window in range(count):
            start = WIN * (first + window)
            if last and window == count - 1:
                right = right_ref[index].astype(F32)
                diag = diag_ref[index].astype(F32)
                top = jnp.concatenate([tile[SHIFT:, start + SHIFT :], right], 1)
                low = jnp.concatenate([below[:, start:], diag], 1)
            else:
                top = tile[SHIFT:, start + SHIFT : start + SHIFT + WIN]
                low = below[:, start : start + WIN]
            both = jnp.concatenate([top, low], 0).reshape(tokens, width)
            target[window * tokens : (window + 1) * tokens, :] = both.astype(target.dtype)

    assemble(token_ref, 0, x_ref)
    assemble(cot_ref, 1, c_ref)

    unit1, scale1 = norm(x_ref[...])
    unit_ref[...] = unit1
    scale_ref[...] = scale1
    normed = (unit1 * gain1_ref[...]).astype(BF16)
    n_ref[...] = normed
    projected = dot(normed, qkv_ref[...], 1, 0)
    q_ref[...] = projected[:, :width]
    k_ref[...] = projected[:, width : 2 * width].astype(BF16)
    v_ref[...] = projected[:, 2 * width :].astype(BF16)
    lane_head = iota((1, width), 1) // head_size
    score_scale = head_size ** (-0.5)

    def of_head(values, head):
        return jnp.where(lane_head == head, values, 0.0).astype(BF16)

    for window in range(count):
        span = slice(window * tokens, (window + 1) * tokens)
        query = q_ref[span, :]
        keys = k_ref[span, :]
        value = v_ref[span, :].astype(F32)
        sources = []
        for head in range(heads):
            scores = dot(of_head(query, head), keys, 1, 1) * (score_scale * LOG2_E)
            scores = scores + bias_ref[first + window, head * tokens : (head + 1) * tokens, :]
            weights = jnp.exp2(scores - jnp.max(scores, axis=-1, keepdims=True))
            p_ref[window, :, head * tokens : (head + 1) * tokens] = weights.astype(BF16)
            ones = jnp.broadcast_to(of_head(jnp.ones((1, width), F32), head), (tokens, width))
            sources.append(jnp.concatenate([of_head(value, head), ones], 1))
        both = dot(p_ref[window], jnp.concatenate(sources, 0), 1, 0)
        inverse = 1.0 / both[:, width:]
        attended = both[:, :width] * inverse
        inverse_ref[span, :] = inverse
        out_f32_ref[span, :] = attended
        att_ref[span, :] = attended.astype(BF16)

    hidden = x_ref[...] + dot(att_ref[...], proj_ref[...], 1, 0).astype(BF16).astype(F32)
    unit2, scale2 = norm(hidden)
    normed2 = (unit2 * gain2_ref[...]).astype(BF16)
    cot = c_ref[...]
    root = math.sqrt(0.5)
    step = 2 * width
    for part in range(hidden_units // step):
        cols = slice(part * step, (part + 1) * step)
        before = dot(normed2, fc1_ref[:, cols], 1, 0)
        normal = 0.5 * (1.0 + lax.erf(before * root))
        inner_ref[:, cols] = (before * normal).astype(BF16)
        density = jnp.exp2(before * before * (-0.5 * LOG2_E)) * (1.0 / math.sqrt(2.0 * math.pi))
        slope = normal + before * density
        grad_inner = dot(cot, fc2_ref[cols, :], 1, 1).astype(BF16).astype(F32)
        before_ref[:, cols] = (grad_inner * slope).astype(BF16)
    inner = inner_ref[...]
    grad_before = before_ref[...]
    out_ref[...] = hidden + dot(inner, fc2_ref[...], 1, 0)
    back = dot(grad_before, fc1_ref[...], 1, 1).astype(BF16).astype(F32)
    grad_fc1 = dot(normed2, grad_before, 0, 0)
    for part in range(hidden_units // width):
        put(part * width, grad_fc1[:, part * width : (part + 1) * width])
    put(hidden_units, dot(inner, cot, 0, 0))
    grad_gain2 = jnp.sum(back * unit2, axis=0, keepdims=True)
    grad_hidden = cot.astype(F32) + norm_back(back * gain2_ref[...], unit2, scale2)
    dh_ref[...] = grad_hidden

    grad_attended = grad_hidden.astype(BF16)
    put(2 * hidden_units + 3 * width, dot(att_ref[...], grad_attended, 0, 0))
    grad_heads = dot(grad_attended, proj_ref[...], 1, 1).astype(BF16).astype(F32)

    minus = jnp.full((tokens, width), -1.0, BF16)
    for window in range(count):
        span = slice(window * tokens, (window + 1) * tokens)
        query = q_ref[span, :]
        keys = k_ref[span, :].astype(F32)
        value = jnp.concatenate([v_ref[span, :], minus], 1)
        scaled = (grad_heads[span, :] * inverse_ref[span, :]).astype(BF16).astype(F32)
        inside = scaled * out_f32_ref[span, :]
        inside_high = inside.astype(BF16).astype(F32)
        inside_low = pltpu.roll(inside - inside_high, head_size, 1)
        query_t = query.T.astype(BF16)
        scaled_t = scaled.T.astype(BF16)
        grad_k, grad_v, sources = [], [], []
        for head in range(heads):
            rows = slice(head * tokens, (head + 1) * tokens)
            part = slice(head * head_size, (head + 1) * head_size)
            extra = jnp.where(
                lane_head == head,
                inside_high,
                jnp.where(lane_head == (head + 1) % heads, inside_low, 0.0),
            ).astype(BF16)
            grad_weights = dot(jnp.concatenate([of_head(scaled, head), extra], 1), value, 1, 1)
            weights = p_ref[window, :, rows]
            grad_scores = grad_weights * weights.astype(F32)
            if window == 0:
                ds_ref[rows, :] = grad_scores
            else:
                ds_ref[rows, :] += grad_scores
            narrow = grad_scores.astype(BF16)
            dsn_ref[:, rows] = narrow
            sources.append(of_head(keys, head))
            grad_k.append(dot(query_t[part, :], narrow, 1, 0))
            grad_v.append(dot(scaled_t[part, :], weights, 1, 0))
        grad_q = dot(dsn_ref[...], jnp.concatenate(sources, 0), 1, 0)
        dqkv_ref[span, :width] = (grad_q * score_scale).astype(BF16)
        grad_k = jnp.concatenate(grad_k, 0).T
        dqkv_ref[span, width : 2 * width] = (grad_k * score_scale).astype(BF16)
        dqkv_ref[span, 2 * width :] = jnp.concatenate(grad_v, 0).T.astype(BF16)

    grad_projected = dqkv_ref[...]
    grad_qkv = dot(n_ref[...], grad_projected, 0, 0)
    for part in range(3):
        put(2 * hidden_units + part * width, grad_qkv[:, part * width : (part + 1) * width])
    grad_normed = dot(grad_projected, qkv_ref[...], 1, 1).astype(BF16).astype(F32)
    unit1 = unit_ref[...]
    grad_gain1 = jnp.sum(grad_normed * unit1, axis=0, keepdims=True)
    grad_x = dh_ref[...] + norm_back(grad_normed * gain1_ref[...], unit1, scale_ref[...])
    gains = jnp.concatenate([grad_gain1, grad_gain2, jnp.zeros((6, width), F32)], 0)

    lanes = 2 * tokens
    rows = heads * WIN
    blank = jnp.zeros((WIN, LANES), F32)
    strip = strip_in[...] if last else jnp.zeros((rows, lanes), F32)
    for fine in range(8):
        near, far = WIN - 1 - fine, WIN - 9 - fine
        blocks = []
        for head in range(heads):
            above = ds_ref[head * tokens + near * WIN : head * tokens + (near + 1) * WIN, :]
            under = ds_ref[head * tokens + far * WIN : head * tokens + (far + 1) * WIN, :]
            blocks.append(
                jnp.concatenate([above, blank, blank], 1) + jnp.concatenate([blank, under, blank], 1)
            )
        block = jnp.concatenate(blocks, 0)
        strip = strip + (pltpu.roll(block, WIN * fine, 1) if fine else block)

    if last:
        finish_table(heads, strip, grads_ref, 2 * hidden_units + 4 * width)
        row = 2 * hidden_units + 4 * width + heads * 2 * WIN
        blank = jnp.zeros((grads_ref.shape[0] - row - 8, width), F32)
        grads_ref[row:, :] = jnp.concatenate([gains_in[...] + gains, blank], 0).astype(BF16)
        half = keep_out.shape[0]
        core = lax.axis_index("group") % 2
        keep_out[...] = grads_ref[pl.ds(pl.multiple_of(core * half, 16), half), :]
        send_out[...] = grads_ref[pl.ds(pl.multiple_of((1 - core) * half, 16), half), :]
    else:
        strip_out[...] = strip
        gains_out[...] = gains

    for index, values in enumerate((out_ref[...], grad_x)):
        for window in range(count):
            start = WIN * window
            block = values[window * tokens : (window + 1) * tokens, :].reshape(WIN, WIN, width)
            top, low = block[:SHIFT], block[SHIFT:]
            if last and window == count - 1:
                own_out[index, :, start:, :] = top[:, :SHIFT].astype(BF16)
                below_out[index, :, start:, :] = low[:, :SHIFT].astype(BF16)
                right_out[index] = top[:, SHIFT:].astype(BF16)
                diag_out[index] = low[:, SHIFT:].astype(BF16)
            else:
                own_out[index, :, start : start + WIN, :] = top.astype(BF16)
                below_out[index, :, start : start + WIN, :] = low.astype(BF16)


def finish_table(heads, strip, grads_ref, row):
    rows, lanes = strip.shape
    lane = iota((rows, lanes), 1)
    amounts = WIN - 1 - iota((rows, lanes), 0) % WIN
    offsets = 2 * WIN
    table = jnp.zeros((heads * offsets, LANES), F32)
    for odd in range(2):
        chosen = jnp.where((lane // WIN) % 2 == odd, strip, 0.0)
        if odd:
            chosen = pltpu.roll(chosen, lanes - WIN, 1)
        chosen = shift_rows(chosen, amounts, True)
        wanted = offsets - 2 - iota((offsets, lanes), 0)
        where_row = (iota((offsets, lanes), 1) // 32) * 2 + odd == wanted
        terms = []
        for head in range(heads):
            flat = jnp.sum(chosen[head * WIN : (head + 1) * WIN, :], axis=0, keepdims=True)
            terms.append(jnp.where(where_row, flat, 0.0))
        terms = jnp.concatenate(terms, 0).astype(BF16)
        pick_lane = iota((lanes, LANES), 0) % 32
        pick = jnp.where(pick_lane == offsets - 2 - iota((lanes, LANES), 1), 1.0, 0.0).astype(BF16)
        table = table + dot(terms, pick, 1, 0)
    grads_ref[row : row + heads * offsets, :] = table.astype(BF16)


def pair_kernel(first_ref, second_ref, out_ref):
    total = first_ref[...].astype(F32) + second_ref[...].astype(F32)
    out_ref[...] = total.astype(out_ref.dtype)


def sum_kernel(in_ref, out_ref):
    total = in_ref[0].astype(F32)
    for index in range(1, in_ref.shape[0]):
        total = total + in_ref[index].astype(F32)
    total = total.astype(out_ref.dtype)
    for index in range(out_ref.shape[0]):
        out_ref[index] = total


def unpack_kernel(
    heads,
    factor,
    mine_ref,
    other_ref,
    gain1_ref,
    qkv_ref,
    proj_ref,
    table_ref,
    gain2_ref,
    fc1_ref,
    fc2_ref,
    summed_ref,
):
    width, hidden_units = fc1_ref.shape
    half = mine_ref.shape[0]
    core = lax.axis_index("group") % 2
    summed_ref[pl.ds(pl.multiple_of(core * half, 16), half), :] = mine_ref[...]
    summed_ref[pl.ds(pl.multiple_of((1 - core) * half, 16), half), :] = other_ref[...]
    offsets = 2 * WIN

    def rows(start, count):
        return summed_ref[start : start + count, :].astype(F32) * factor

    for part in range(hidden_units // width):
        fc1_ref[:, part * width : (part + 1) * width] = rows(part * width, width)
    fc2_ref[...] = rows(hidden_units, hidden_units)
    for part in range(3):
        qkv_ref[:, part * width : (part + 1) * width] = rows(2 * hidden_units + part * width, width)
    start = 2 * hidden_units + 3 * width
    proj_ref[...] = rows(start, width)
    start = start + width
    for head in range(heads):
        block = rows(start + head * offsets, offsets)
        table_ref[:, head, :] = block[: offsets - 1, : offsets - 1]
    start = start + heads * offsets
    gains = rows(start, 16)
    gain1_ref[...] = gains[0:1]
    gain2_ref[...] = gains[1:2]


def neighbour_pairs(row_step, col_step):
    groups, tiles = lax.axis_size("group"), lax.axis_size("tile")
    pairs = []
    for group in range(groups):
        for tile in range(tiles):
            target = ((group + row_step) % groups) * tiles + (tile + col_step) % tiles
            pairs.append((group * tiles + tile, target))
    return pairs


def passed_along(value, row_step, col_step):
    return lax.ppermute(value, AXES, neighbour_pairs(row_step, col_step))


def shards(tokens, gain1, w_qkv, w_proj, bias_table, gain2, w_fc1, w_fc2, cotangent):
    row_count, col_count, width = tokens.shape
    heads = bias_table.shape[0]
    hidden_units = w_fc1.shape[1]
    groups, tiles = lax.axis_size("group"), lax.axis_size("tile")
    devices = groups * tiles
    windows = col_count // WIN
    token_count = WIN * WIN
    keep = col_count - SHIFT

    vmem = pl.BlockSpec(memory_space=pltpu.VMEM)

    def array(shape, dtype=BF16):
        return jax.ShapeDtypeStruct(shape, dtype)

    below, right, diag = pl.pallas_call(
        cut_kernel,
        out_shape=(
            array((2, SHIFT, keep, width)),
            array((2, SHIFT, SHIFT, width)),
            array((2, SHIFT, SHIFT, width)),
        ),
        in_specs=[vmem] * 2,
        out_specs=(vmem,) * 3,
        name="cut",
        compiler_params=PARAMS,
    )(tokens, cotangent)
    below = passed_along(below, -1, 0)
    right = passed_along(right, 0, -1)
    diag = passed_along(diag, -1, -1)

    bias = pl.pallas_call(
        functools.partial(bias_kernel, heads, windows),
        out_shape=jax.ShapeDtypeStruct((windows, heads * token_count, token_count), F32),
        in_specs=[vmem],
        out_specs=vmem,
        name="bias",
        compiler_params=PARAMS,
        cost_estimate=pl.CostEstimate(flops=8_000_000, bytes_accessed=2_000_000, transcendentals=0),
    )(bias_table.transpose(1, 0, 2))

    used = 2 * hidden_units + 4 * width + heads * 2 * WIN + 16
    members = devices // 2
    chunk = (used + devices * 8 - 1) // (devices * 8) * 8
    half = chunk * members
    weights = (gain1.reshape(1, width), w_qkv, w_proj, gain2.reshape(1, width), w_fc1, w_fc2)
    sum_rows = 2 * hidden_units + 4 * width

    def block(first, count, last, inputs, outputs):
        total = count * token_count
        scratch = [
            pltpu.VMEM((total, width), F32),
            pltpu.VMEM((total, width), BF16),
            pltpu.VMEM((total, width), BF16),
            pltpu.VMEM((total, width), F32),
            pltpu.VMEM((total, 1), F32),
            pltpu.VMEM((total, width), F32),
            pltpu.VMEM((total, width), BF16),
            pltpu.VMEM((total, width), BF16),
            pltpu.VMEM((count, token_count, heads * token_count), BF16),
            pltpu.VMEM((total, width), BF16),
            pltpu.VMEM((total, width), F32),
            pltpu.VMEM((total, width), F32),
            pltpu.VMEM((total, width), F32),
            pltpu.VMEM((total, 3 * width), BF16),
            pltpu.VMEM((heads * token_count, token_count), F32),
            pltpu.VMEM((token_count, heads * token_count), BF16),
            pltpu.VMEM((total, hidden_units), BF16),
            pltpu.VMEM((total, hidden_units), BF16),
            pltpu.VMEM((total, width), F32),
        ]
        if last:
            scratch = [pltpu.VMEM((2 * half, width), BF16)] + scratch
        inputs = inputs + (bias,) + weights
        return pl.pallas_call(
            functools.partial(block_kernel, heads, first, count, last),
            out_shape=outputs,
            in_specs=[vmem] * len(inputs),
            out_specs=(vmem,) * len(outputs),
            scratch_shapes=scratch,
            name="last" if last else "first",
            compiler_params=PARAMS,
            cost_estimate=pl.CostEstimate(
                flops=1_000_000_000 * count, bytes_accessed=2_000_000, transcendentals=1_000_000
            ),
        )(*inputs)

    early = WIN * (windows - 1)
    own_first, below_first, sums, strip, gains = block(
        0,
        windows - 1,
        False,
        (tokens, cotangent, below),
        (
            array((2, SHIFT, early, width)),
            array((2, SHIFT, early, width)),
            array((sum_rows, width), F32),
            array((heads * WIN, 2 * token_count), F32),
            array((8, width), F32),
        ),
    )
    back_first = passed_along(below_first, 1, 0)
    own_last, below_last, right_last, diag_last, kept, sent = block(
        windows - 1,
        1,
        True,
        (tokens, cotangent, below, right, diag, sums, strip, gains),
        (
            array((2, SHIFT, SHIFT, width)),
            array((2, SHIFT, SHIFT, width)),
            array((2, SHIFT, SHIFT, width)),
            array((2, SHIFT, SHIFT, width)),
            array((half, width)),
            array((half, width)),
        ),
    )
    back_below = passed_along(below_last, 1, 0)
    back_right = passed_along(right_last, 0, 1)
    back_diag = passed_along(diag_last, 1, 1)

    pairs = [(index, index + tiles if index // tiles % 2 == 0 else index - tiles) for index in range(devices)]
    same_core = [
        [index for index in range(devices) if index // tiles % 2 == core] for core in range(2)
    ]

    def exchanged(value):
        return lax.all_to_all(value, AXES, 0, 0, tiled=True, axis_index_groups=same_core)

    received = lax.ppermute(sent, AXES, pairs)
    paired = pl.pallas_call(
        pair_kernel,
        out_shape=jax.ShapeDtypeStruct((half, width), BF16),
        in_specs=[vmem] * 2,
        out_specs=vmem,
        name="pair",
        compiler_params=PARAMS,
    )(kept, received)
    copies = pl.pallas_call(
        sum_kernel,
        out_shape=jax.ShapeDtypeStruct((members, chunk, width), BF16),
        in_specs=[vmem],
        out_specs=vmem,
        name="add",
        compiler_params=PARAMS,
    )(exchanged(paired.reshape(members, chunk, width)))
    mine = exchanged(copies).reshape(half, width)
    other = lax.ppermute(mine, AXES, pairs)

    factor = 1.0 / math.sqrt(row_count * groups * col_count * tiles)
    grad_gain1, grad_qkv, grad_proj, grad_table, grad_gain2, grad_fc1, grad_fc2 = pl.pallas_call(
        functools.partial(unpack_kernel, heads, factor),
        out_shape=(
            jax.ShapeDtypeStruct((1, width), F32),
            jax.ShapeDtypeStruct(w_qkv.shape, F32),
            jax.ShapeDtypeStruct(w_proj.shape, F32),
            jax.ShapeDtypeStruct((bias_table.shape[1], heads, bias_table.shape[2]), F32),
            jax.ShapeDtypeStruct((1, width), F32),
            jax.ShapeDtypeStruct(w_fc1.shape, F32),
            jax.ShapeDtypeStruct(w_fc2.shape, F32),
        ),
        in_specs=[vmem] * 2,
        out_specs=(vmem,) * 7,
        scratch_shapes=[pltpu.VMEM((2 * half, width), BF16)],
        name="unpack",
        compiler_params=PARAMS,
    )(mine, other)

    high = jnp.concatenate([back_diag, back_first, back_below], 2)
    low = jnp.concatenate([back_right, own_first, own_last], 2)
    whole = jnp.concatenate([high, low], 1)
    return (
        whole[0],
        whole[1],
        grad_gain1.reshape(width),
        grad_qkv,
        grad_proj,
        grad_table.transpose(1, 0, 2),
        grad_gain2.reshape(width),
        grad_fc1,
        grad_fc2,
    )


def solution(mesh):
    tile_spec = P("group", "tile", None)
    return jax.shard_map(
        shards,
        mesh=mesh,
        in_specs=(tile_spec, P(), P(), P(), P(), P(), P(), P(), tile_spec),
        out_specs=(tile_spec, tile_spec, P(), P(), P(), P(), P(), P(), P()),
        check_vma=False,
    )
```

```python
import functools
import math

import jax
import jax.numpy as jnp
from jax import lax
from jax.experimental import pallas as pl
from jax.experimental.pallas import tpu as pltpu
from jax.sharding import PartitionSpec as P

WIN = 16
SHIFT = 8
NORM_EPS = 1e-05
LOG2_E = math.log2(math.e)
LANES = 128
F32 = jnp.float32
BF16 = jnp.bfloat16
AXES = ("group", "tile")
PARAMS = pltpu.CompilerParams(vmem_limit_bytes=24 * 1024 * 1024)


def dot(left, right, left_dim, right_dim, precision=None):
    return lax.dot_general(
        left,
        right,
        (((left_dim,), (right_dim,)), ((), ())),
        preferred_element_type=F32,
        precision=precision,
    )


def iota(shape, dim):
    return lax.broadcasted_iota(jnp.int32, shape, dim)


def shift_rows(values, amounts, right):
    width = values.shape[1]
    for bit in range(4):
        step = 1 << bit
        moved = pltpu.roll(values, step if right else width - step, 1)
        values = jnp.where((amounts & step) != 0, moved, values)
    return values


def bias_kernel(heads, windows, table_ref, out_ref, pad_ref):
    span = 2 * WIN * WIN
    tokens = WIN * WIN
    offsets = 2 * WIN - 1
    block = offsets + 1
    pad_ref[...] = jnp.zeros_like(pad_ref)
    for head in range(heads):
        pad_ref[head * block : head * block + offsets, :offsets] = table_ref[:, head, :]
    padded = pad_ref[...]
    parts = []
    for _ in range(3):
        part = padded.astype(BF16)
        parts.append(part)
        padded = padded - part.astype(F32)
    chosen = iota((LANES, span), 1) % 32 == offsets - 1 - iota((LANES, span), 0)
    spread = dot(jnp.concatenate(parts, 0), jnp.where(chosen, 1.0, 0.0).astype(BF16), 1, 0)
    size = heads * block
    spread = spread[:size] + spread[size : 2 * size] + spread[2 * size :]
    flats = []
    for odd in range(2):
        wanted = offsets - 1 - iota((block, span), 0)
        keep = (iota((block, span), 1) // 32) * 2 + odd == wanted
        for head in range(heads):
            mine = spread[head * block : (head + 1) * block]
            flat = jnp.sum(jnp.where(keep, mine, 0.0), axis=0, keepdims=True)
            flats.append(jnp.broadcast_to(flat, (WIN, span)))
    rows = heads * WIN
    amounts = WIN - 1 - iota((rows, span), 0) % WIN
    even = shift_rows(jnp.concatenate(flats[:heads], 0), amounts, False)
    odd = shift_rows(jnp.concatenate(flats[heads:], 0), amounts, False)
    odd = pltpu.roll(odd, WIN, 1)
    strip = jnp.where(iota((rows, span), 1) % 32 < WIN, even, odd) * LOG2_E
    last_row = (lax.axis_index("group") == lax.axis_size("group") - 1).astype(jnp.int32)
    last_col = (lax.axis_index("tile") == lax.axis_size("tile") - 1).astype(jnp.int32)
    key = iota((WIN, tokens), 1)
    query_x = iota((WIN, tokens), 0)
    key_low = (key >= tokens // 2).astype(jnp.int32)
    cross_col = ((key % WIN >= SHIFT) != (query_x >= SHIFT)).astype(jnp.int32)
    for fine in range(8):
        moved = pltpu.roll(strip, (span - WIN * fine) % span, 1)
        for coarse in range(2):
            y = WIN - 1 - (8 * coarse + fine)
            cross_row = key_low if y < SHIFT else 1 - key_low
            for window in range(windows):
                apart = cross_row * last_row
                if window == windows - 1:
                    apart = apart + cross_col * last_col
                extra = jnp.where(apart > 0, -1e30, 0.0)
                for head in range(heads):
                    part = moved[
                        head * WIN : (head + 1) * WIN,
                        LANES * coarse : LANES * coarse + tokens,
                    ]
                    start = head * tokens + y * WIN
                    out_ref[window, start : start + WIN, :] = part + extra


def mean_of(values):
    return jnp.mean(values, axis=-1, keepdims=True)


def norm(values):
    centred = values - mean_of(values)
    scale = lax.rsqrt(mean_of(centred * centred) + NORM_EPS)
    return centred * scale, scale


def norm_back(grad, unit, scale):
    return scale * (grad - mean_of(grad) - unit * mean_of(grad * unit))


def cut_kernel(token_ref, cot_ref, table_ref, below_ref, right_ref, diag_ref, table_out, sems):
    copies = []

    def copy(source, target):
        copies.append(pltpu.make_async_copy(source, target, sems.at[len(copies)]))

    high, low = pl.ds(0, SHIFT), pl.ds(SHIFT, SHIFT)
    rest = pl.ds(SHIFT, token_ref.shape[1] - SHIFT)
    for index, tile_ref in enumerate((token_ref, cot_ref)):
        copy(tile_ref.at[high, rest], below_ref.at[index])
        copy(tile_ref.at[low, high], right_ref.at[index])
        copy(tile_ref.at[high, high], diag_ref.at[index])
    copy(table_ref, table_out)
    for each in copies:
        each.start()
    for each in copies:
        each.wait()


def block_kernel(heads, first, count, last, *refs):
    token_ref, cot_ref, below_ref = refs[:3]
    refs = refs[3:]
    if last:
        right_ref, diag_ref, sums_in, strip_in, gains_in = refs[:5]
        refs = refs[5:]
    bias_ref, gain1_ref, qkv_ref, proj_ref, gain2_ref, fc1_ref, fc2_ref = refs[:7]
    own_out, below_out = refs[7:9]
    refs = refs[9:]
    if last:
        right_out, diag_out, keep_out, send_out, grads_ref = refs[:5]
        refs = refs[5:]
    else:
        sums_out, strip_out, gains_out = refs[:3]
        refs = refs[3:]
    x_ref, c_ref, n_ref, unit_ref, scale_ref, q_ref, k_ref, v_ref = refs[:8]
    p_ref, att_ref, out_f32_ref, inverse_ref, dh_ref, dqkv_ref, ds_ref, dsn_ref = refs[8:16]
    inner_ref, before_ref, out_ref = refs[16:]

    tokens = WIN * WIN
    width = token_ref.shape[2]
    head_size = width // heads
    total = count * tokens
    hidden_units = fc1_ref.shape[1]

    def put(row, value):
        rows = slice(row, row + value.shape[0])
        if last:
            grads_ref[rows, :] = (sums_in[rows, :] + value).astype(BF16)
        else:
            sums_out[rows, :] = value

    def assemble(tile_ref, index, target):
        tile = tile_ref[...].astype(F32)
        below = below_ref[index].astype(F32)
        for window in range(count):
            start = WIN * (first + window)
            if last and window == count - 1:
                right = right_ref[index].astype(F32)
                diag = diag_ref[index].astype(F32)
                top = jnp.concatenate([tile[SHIFT:, start + SHIFT :], right], 1)
                low = jnp.concatenate([below[:, start:], diag], 1)
            else:
                top = tile[SHIFT:, start + SHIFT : start + SHIFT + WIN]
                low = below[:, start : start + WIN]
            both = jnp.concatenate([top, low], 0).reshape(tokens, width)
            target[window * tokens : (window + 1) * tokens, :] = both.astype(target.dtype)

    assemble(token_ref, 0, x_ref)
    assemble(cot_ref, 1, c_ref)

    unit1, scale1 = norm(x_ref[...])
    unit_ref[...] = unit1
    scale_ref[...] = scale1
    normed = (unit1 * gain1_ref[...]).astype(BF16)
    n_ref[...] = normed
    projected = dot(normed, qkv_ref[...], 1, 0)
    q_ref[...] = projected[:, :width]
    k_ref[...] = projected[:, width : 2 * width].astype(BF16)
    v_ref[...] = projected[:, 2 * width :].astype(BF16)
    lane_head = iota((1, width), 1) // head_size
    score_scale = head_size ** (-0.5)

    def of_head(values, head):
        return jnp.where(lane_head == head, values, 0.0).astype(BF16)

    for window in range(count):
        span = slice(window * tokens, (window + 1) * tokens)
        query = q_ref[span, :]
        keys = k_ref[span, :]
        value = v_ref[span, :].astype(F32)
        sources = []
        for head in range(heads):
            scores = dot(of_head(query, head), keys, 1, 1) * (score_scale * LOG2_E)
            scores = scores + bias_ref[first + window, head * tokens : (head + 1) * tokens, :]
            weights = jnp.exp2(scores - jnp.max(scores, axis=-1, keepdims=True))
            p_ref[window, :, head * tokens : (head + 1) * tokens] = weights.astype(BF16)
            ones = jnp.broadcast_to(of_head(jnp.ones((1, width), F32), head), (tokens, width))
            sources.append(jnp.concatenate([of_head(value, head), ones], 1))
        both = dot(p_ref[window], jnp.concatenate(sources, 0), 1, 0)
        inverse = 1.0 / both[:, width:]
        attended = both[:, :width] * inverse
        inverse_ref[span, :] = inverse
        out_f32_ref[span, :] = attended
        att_ref[span, :] = attended.astype(BF16)

    hidden = x_ref[...] + dot(att_ref[...], proj_ref[...], 1, 0).astype(BF16).astype(F32)
    unit2, scale2 = norm(hidden)
    normed2 = (unit2 * gain2_ref[...]).astype(BF16)
    cot = c_ref[...]
    root = math.sqrt(0.5)
    step = 2 * width
    for part in range(hidden_units // step):
        cols = slice(part * step, (part + 1) * step)
        before = dot(normed2, fc1_ref[:, cols], 1, 0)
        normal = 0.5 * (1.0 + lax.erf(before * root))
        inner_ref[:, cols] = (before * normal).astype(BF16)
        density = jnp.exp2(before * before * (-0.5 * LOG2_E)) * (1.0 / math.sqrt(2.0 * math.pi))
        slope = normal + before * density
        grad_inner = dot(cot, fc2_ref[cols, :], 1, 1).astype(BF16).astype(F32)
        before_ref[:, cols] = (grad_inner * slope).astype(BF16)
    inner = inner_ref[...]
    grad_before = before_ref[...]
    out_ref[...] = hidden + dot(inner, fc2_ref[...], 1, 0)
    back = dot(grad_before, fc1_ref[...], 1, 1).astype(BF16).astype(F32)
    grad_fc1 = dot(normed2, grad_before, 0, 0)
    for part in range(hidden_units // width):
        put(part * width, grad_fc1[:, part * width : (part + 1) * width])
    put(hidden_units, dot(inner, cot, 0, 0))
    grad_gain2 = jnp.sum(back * unit2, axis=0, keepdims=True)
    grad_hidden = cot.astype(F32) + norm_back(back * gain2_ref[...], unit2, scale2)
    dh_ref[...] = grad_hidden

    grad_attended = grad_hidden.astype(BF16)
    put(2 * hidden_units + 3 * width, dot(att_ref[...], grad_attended, 0, 0))
    grad_heads = dot(grad_attended, proj_ref[...], 1, 1).astype(BF16).astype(F32)

    minus = jnp.full((tokens, width), -1.0, BF16)
    for window in range(count):
        span = slice(window * tokens, (window + 1) * tokens)
        query = q_ref[span, :]
        keys = k_ref[span, :].astype(F32)
        value = jnp.concatenate([v_ref[span, :], minus], 1)
        scaled = (grad_heads[span, :] * inverse_ref[span, :]).astype(BF16).astype(F32)
        inside = scaled * out_f32_ref[span, :]
        inside_high = inside.astype(BF16).astype(F32)
        inside_low = pltpu.roll(inside - inside_high, head_size, 1)
        query_t = query.T.astype(BF16)
        scaled_t = scaled.T.astype(BF16)
        grad_k, grad_v, sources = [], [], []
        for head in range(heads):
            rows = slice(head * tokens, (head + 1) * tokens)
            part = slice(head * head_size, (head + 1) * head_size)
            extra = jnp.where(
                lane_head == head,
                inside_high,
                jnp.where(lane_head == (head + 1) % heads, inside_low, 0.0),
            ).astype(BF16)
            grad_weights = dot(jnp.concatenate([of_head(scaled, head), extra], 1), value, 1, 1)
            weights = p_ref[window, :, rows]
            grad_scores = grad_weights * weights.astype(F32)
            if window == 0:
                ds_ref[rows, :] = grad_scores
            else:
                ds_ref[rows, :] += grad_scores
            narrow = grad_scores.astype(BF16)
            dsn_ref[:, rows] = narrow
            sources.append(of_head(keys, head))
            grad_k.append(dot(query_t[part, :], narrow, 1, 0))
            grad_v.append(dot(scaled_t[part, :], weights, 1, 0))
        grad_q = dot(dsn_ref[...], jnp.concatenate(sources, 0), 1, 0)
        dqkv_ref[span, :width] = (grad_q * score_scale).astype(BF16)
        grad_k = jnp.concatenate(grad_k, 0).T
        dqkv_ref[span, width : 2 * width] = (grad_k * score_scale).astype(BF16)
        dqkv_ref[span, 2 * width :] = jnp.concatenate(grad_v, 0).T.astype(BF16)

    grad_projected = dqkv_ref[...]
    grad_qkv = dot(n_ref[...], grad_projected, 0, 0)
    for part in range(3):
        put(2 * hidden_units + part * width, grad_qkv[:, part * width : (part + 1) * width])
    grad_normed = dot(grad_projected, qkv_ref[...], 1, 1).astype(BF16).astype(F32)
    unit1 = unit_ref[...]
    grad_gain1 = jnp.sum(grad_normed * unit1, axis=0, keepdims=True)
    grad_x = dh_ref[...] + norm_back(grad_normed * gain1_ref[...], unit1, scale_ref[...])
    gains = jnp.concatenate([grad_gain1, grad_gain2, jnp.zeros((6, width), F32)], 0)

    lanes = 2 * tokens
    rows = heads * WIN
    blank = jnp.zeros((WIN, LANES), F32)
    strip = strip_in[...] if last else jnp.zeros((rows, lanes), F32)
    for fine in range(8):
        near, far = WIN - 1 - fine, WIN - 9 - fine
        blocks = []
        for head in range(heads):
            above = ds_ref[head * tokens + near * WIN : head * tokens + (near + 1) * WIN, :]
            under = ds_ref[head * tokens + far * WIN : head * tokens + (far + 1) * WIN, :]
            blocks.append(
                jnp.concatenate([above, blank, blank], 1) + jnp.concatenate([blank, under, blank], 1)
            )
        block = jnp.concatenate(blocks, 0)
        strip = strip + (pltpu.roll(block, WIN * fine, 1) if fine else block)

    if last:
        finish_table(heads, strip, grads_ref, 2 * hidden_units + 4 * width)
        row = 2 * hidden_units + 4 * width + heads * 2 * WIN
        blank = jnp.zeros((grads_ref.shape[0] - row - 8, width), F32)
        grads_ref[row:, :] = jnp.concatenate([gains_in[...] + gains, blank], 0).astype(BF16)
        half = keep_out.shape[0]
        core = lax.axis_index("group") % 2
        keep_out[...] = grads_ref[pl.ds(pl.multiple_of(core * half, 16), half), :]
        send_out[...] = grads_ref[pl.ds(pl.multiple_of((1 - core) * half, 16), half), :]
    else:
        strip_out[...] = strip
        gains_out[...] = gains

    for index, values in enumerate((out_ref[...], grad_x)):
        for window in range(count):
            start = WIN * window
            block = values[window * tokens : (window + 1) * tokens, :].reshape(WIN, WIN, width)
            top, low = block[:SHIFT], block[SHIFT:]
            if last and window == count - 1:
                own_out[index, :, start:, :] = top[:, :SHIFT].astype(BF16)
                below_out[index, :, start:, :] = low[:, :SHIFT].astype(BF16)
                right_out[index] = top[:, SHIFT:].astype(BF16)
                diag_out[index] = low[:, SHIFT:].astype(BF16)
            else:
                own_out[index, :, start : start + WIN, :] = top.astype(BF16)
                below_out[index, :, start : start + WIN, :] = low.astype(BF16)


def finish_table(heads, strip, grads_ref, row):
    rows, lanes = strip.shape
    lane = iota((rows, lanes), 1)
    amounts = WIN - 1 - iota((rows, lanes), 0) % WIN
    offsets = 2 * WIN
    table = jnp.zeros((heads * offsets, LANES), F32)
    for odd in range(2):
        chosen = jnp.where((lane // WIN) % 2 == odd, strip, 0.0)
        if odd:
            chosen = pltpu.roll(chosen, lanes - WIN, 1)
        chosen = shift_rows(chosen, amounts, True)
        wanted = offsets - 2 - iota((offsets, lanes), 0)
        where_row = (iota((offsets, lanes), 1) // 32) * 2 + odd == wanted
        terms = []
        for head in range(heads):
            flat = jnp.sum(chosen[head * WIN : (head + 1) * WIN, :], axis=0, keepdims=True)
            terms.append(jnp.where(where_row, flat, 0.0))
        terms = jnp.concatenate(terms, 0).astype(BF16)
        pick_lane = iota((lanes, LANES), 0) % 32
        pick = jnp.where(pick_lane == offsets - 2 - iota((lanes, LANES), 1), 1.0, 0.0).astype(BF16)
        table = table + dot(terms, pick, 1, 0)
    grads_ref[row : row + heads * offsets, :] = table.astype(BF16)


def pair_kernel(first_ref, second_ref, out_ref):
    total = first_ref[...].astype(F32) + second_ref[...].astype(F32)
    out_ref[...] = total.astype(out_ref.dtype)


def sum_kernel(in_ref, out_ref):
    total = in_ref[0].astype(F32)
    for index in range(1, in_ref.shape[0]):
        total = total + in_ref[index].astype(F32)
    total = total.astype(out_ref.dtype)
    for index in range(out_ref.shape[0]):
        out_ref[index] = total


def unpack_kernel(
    heads,
    factor,
    mine_ref,
    other_ref,
    diag_ref,
    above_first_ref,
    above_last_ref,
    left_ref,
    own_first_ref,
    own_last_ref,
    out_ref,
    grad_ref,
    gain1_ref,
    qkv_ref,
    proj_ref,
    table_ref,
    gain2_ref,
    fc1_ref,
    fc2_ref,
    summed_ref,
):
    width, hidden_units = fc1_ref.shape
    half = mine_ref.shape[0]
    early = own_first_ref.shape[2]
    for index, target in enumerate((out_ref, grad_ref)):
        target[:SHIFT, :SHIFT, :] = diag_ref[index]
        target[:SHIFT, SHIFT : SHIFT + early, :] = above_first_ref[index]
        target[:SHIFT, SHIFT + early :, :] = above_last_ref[index]
        target[SHIFT:, :SHIFT, :] = left_ref[index]
        target[SHIFT:, SHIFT : SHIFT + early, :] = own_first_ref[index]
        target[SHIFT:, SHIFT + early :, :] = own_last_ref[index]
    core = lax.axis_index("group") % 2
    summed_ref[pl.ds(pl.multiple_of(core * half, 16), half), :] = mine_ref[...]
    summed_ref[pl.ds(pl.multiple_of((1 - core) * half, 16), half), :] = other_ref[...]
    offsets = 2 * WIN

    def rows(start, count):
        return summed_ref[start : start + count, :].astype(F32) * factor

    for part in range(hidden_units // width):
        fc1_ref[:, part * width : (part + 1) * width] = rows(part * width, width)
    fc2_ref[...] = rows(hidden_units, hidden_units)
    for part in range(3):
        qkv_ref[:, part * width : (part + 1) * width] = rows(2 * hidden_units + part * width, width)
    start = 2 * hidden_units + 3 * width
    proj_ref[...] = rows(start, width)
    start = start + width
    for head in range(heads):
        block = rows(start + head * offsets, offsets)
        table_ref[:, head, :] = block[: offsets - 1, : offsets - 1]
    start = start + heads * offsets
    gains = rows(start, 16)
    gain1_ref[...] = gains[0:1]
    gain2_ref[...] = gains[1:2]


def neighbour_pairs(row_step, col_step):
    groups, tiles = lax.axis_size("group"), lax.axis_size("tile")
    pairs = []
    for group in range(groups):
        for tile in range(tiles):
            target = ((group + row_step) % groups) * tiles + (tile + col_step) % tiles
            pairs.append((group * tiles + tile, target))
    return pairs


def passed_along(value, row_step, col_step):
    return lax.ppermute(value, AXES, neighbour_pairs(row_step, col_step))


def shards(tokens, gain1, w_qkv, w_proj, bias_table, gain2, w_fc1, w_fc2, cotangent):
    row_count, col_count, width = tokens.shape
    heads = bias_table.shape[0]
    hidden_units = w_fc1.shape[1]
    groups, tiles = lax.axis_size("group"), lax.axis_size("tile")
    devices = groups * tiles
    windows = col_count // WIN
    token_count = WIN * WIN
    keep = col_count - SHIFT

    vmem = pl.BlockSpec(memory_space=pltpu.VMEM)

    def array(shape, dtype=BF16):
        return jax.ShapeDtypeStruct(shape, dtype)

    table = bias_table.transpose(1, 0, 2)
    hbm = pl.BlockSpec(memory_space=pltpu.HBM)
    below, right, diag, table = pl.pallas_call(
        cut_kernel,
        out_shape=(
            array((2, SHIFT, keep, width)),
            array((2, SHIFT, SHIFT, width)),
            array((2, SHIFT, SHIFT, width)),
            array(table.shape, F32),
        ),
        in_specs=[hbm] * 3,
        out_specs=(vmem,) * 4,
        scratch_shapes=[pltpu.SemaphoreType.DMA((7,))],
        name="cut",
        compiler_params=PARAMS,
    )(*(pltpu.with_memory_space_constraint(each, pltpu.HBM) for each in (tokens, cotangent, table)))
    below = passed_along(below, -1, 0)
    right = passed_along(right, 0, -1)
    diag = passed_along(diag, -1, -1)

    bias = pl.pallas_call(
        functools.partial(bias_kernel, heads, windows),
        out_shape=jax.ShapeDtypeStruct((windows, heads * token_count, token_count), F32),
        in_specs=[vmem],
        out_specs=vmem,
        scratch_shapes=[pltpu.VMEM((heads * 2 * WIN, LANES), F32)],
        name="bias",
        compiler_params=PARAMS,
        cost_estimate=pl.CostEstimate(flops=8_000_000, bytes_accessed=2_000_000, transcendentals=0),
    )(table)

    used = 2 * hidden_units + 4 * width + heads * 2 * WIN + 16
    members = devices // 2
    chunk = (used + devices * 8 - 1) // (devices * 8) * 8
    half = chunk * members
    weights = (gain1.reshape(1, width), w_qkv, w_proj, gain2.reshape(1, width), w_fc1, w_fc2)
    sum_rows = 2 * hidden_units + 4 * width

    def block(first, count, last, inputs, outputs):
        total = count * token_count
        scratch = [
            pltpu.VMEM((total, width), F32),
            pltpu.VMEM((total, width), BF16),
            pltpu.VMEM((total, width), BF16),
            pltpu.VMEM((total, width), F32),
            pltpu.VMEM((total, 1), F32),
            pltpu.VMEM((total, width), F32),
            pltpu.VMEM((total, width), BF16),
            pltpu.VMEM((total, width), BF16),
            pltpu.VMEM((count, token_count, heads * token_count), BF16),
            pltpu.VMEM((total, width), BF16),
            pltpu.VMEM((total, width), F32),
            pltpu.VMEM((total, width), F32),
            pltpu.VMEM((total, width), F32),
            pltpu.VMEM((total, 3 * width), BF16),
            pltpu.VMEM((heads * token_count, token_count), F32),
            pltpu.VMEM((token_count, heads * token_count), BF16),
            pltpu.VMEM((total, hidden_units), BF16),
            pltpu.VMEM((total, hidden_units), BF16),
            pltpu.VMEM((total, width), F32),
        ]
        if last:
            scratch = [pltpu.VMEM((2 * half, width), BF16)] + scratch
        inputs = inputs + (bias,) + weights
        return pl.pallas_call(
            functools.partial(block_kernel, heads, first, count, last),
            out_shape=outputs,
            in_specs=[vmem] * len(inputs),
            out_specs=(vmem,) * len(outputs),
            scratch_shapes=scratch,
            name="last" if last else "first",
            compiler_params=PARAMS,
            cost_estimate=pl.CostEstimate(
                flops=1_000_000_000 * count, bytes_accessed=2_000_000, transcendentals=1_000_000
            ),
        )(*inputs)

    early = WIN * (windows - 1)
    own_first, below_first, sums, strip, gains = block(
        0,
        windows - 1,
        False,
        (tokens, cotangent, below),
        (
            array((2, SHIFT, early, width)),
            array((2, SHIFT, early, width)),
            array((sum_rows, width), F32),
            array((heads * WIN, 2 * token_count), F32),
            array((8, width), F32),
        ),
    )
    back_first = passed_along(below_first, 1, 0)
    own_last, below_last, right_last, diag_last, kept, sent = block(
        windows - 1,
        1,
        True,
        (tokens, cotangent, below, right, diag, sums, strip, gains),
        (
            array((2, SHIFT, SHIFT, width)),
            array((2, SHIFT, SHIFT, width)),
            array((2, SHIFT, SHIFT, width)),
            array((2, SHIFT, SHIFT, width)),
            array((half, width)),
            array((half, width)),
        ),
    )
    back_below = passed_along(below_last, 1, 0)
    back_right = passed_along(right_last, 0, 1)
    back_diag = passed_along(diag_last, 1, 1)

    pairs = [(index, index + tiles if index // tiles % 2 == 0 else index - tiles) for index in range(devices)]
    same_core = [
        [index for index in range(devices) if index // tiles % 2 == core] for core in range(2)
    ]

    def exchanged(value):
        return lax.all_to_all(value, AXES, 0, 0, tiled=True, axis_index_groups=same_core)

    received = lax.ppermute(sent, AXES, pairs)
    paired = pl.pallas_call(
        pair_kernel,
        out_shape=jax.ShapeDtypeStruct((half, width), BF16),
        in_specs=[vmem] * 2,
        out_specs=vmem,
        name="pair",
        compiler_params=PARAMS,
    )(kept, received)
    copies = pl.pallas_call(
        sum_kernel,
        out_shape=jax.ShapeDtypeStruct((members, chunk, width), BF16),
        in_specs=[vmem],
        out_specs=vmem,
        name="add",
        compiler_params=PARAMS,
    )(exchanged(paired.reshape(members, chunk, width)))
    copies, back_first, back_below, back_right, back_diag = lax.optimization_barrier(
        (copies, back_first, back_below, back_right, back_diag)
    )
    mine = exchanged(copies).reshape(half, width)
    other = lax.ppermute(mine, AXES, pairs)

    factor = 1.0 / math.sqrt(row_count * groups * col_count * tiles)
    (
        block_output,
        grad_tokens,
        grad_gain1,
        grad_qkv,
        grad_proj,
        grad_table,
        grad_gain2,
        grad_fc1,
        grad_fc2,
    ) = pl.pallas_call(
        functools.partial(unpack_kernel, heads, factor),
        out_shape=(
            array(tokens.shape),
            array(tokens.shape),
            jax.ShapeDtypeStruct((1, width), F32),
            jax.ShapeDtypeStruct(w_qkv.shape, F32),
            jax.ShapeDtypeStruct(w_proj.shape, F32),
            jax.ShapeDtypeStruct((bias_table.shape[1], heads, bias_table.shape[2]), F32),
            jax.ShapeDtypeStruct((1, width), F32),
            jax.ShapeDtypeStruct(w_fc1.shape, F32),
            jax.ShapeDtypeStruct(w_fc2.shape, F32),
        ),
        in_specs=[vmem] * 8,
        out_specs=(vmem,) * 9,
        scratch_shapes=[pltpu.VMEM((2 * half, width), BF16)],
        name="unpack",
        compiler_params=PARAMS,
    )(mine, other, back_diag, back_first, back_below, back_right, own_first, own_last)

    return (
        block_output,
        grad_tokens,
        grad_gain1.reshape(width),
        grad_qkv,
        grad_proj,
        grad_table.transpose(1, 0, 2),
        grad_gain2.reshape(width),
        grad_fc1,
        grad_fc2,
    )


def solution(mesh):
    tile_spec = P("group", "tile", None)
    return jax.shard_map(
        shards,
        mesh=mesh,
        in_specs=(tile_spec, P(), P(), P(), P(), P(), P(), P(), tile_spec),
        out_specs=(tile_spec, tile_spec, P(), P(), P(), P(), P(), P(), P()),
        check_vma=False,
    )
```

```python
import functools
import math

import jax
import jax.numpy as jnp
from jax import lax
from jax.experimental import pallas as pl
from jax.experimental.pallas import tpu as pltpu
from jax.sharding import PartitionSpec as P


WIN = 16
SHIFT = 8
NORM_EPS = 1e-05
LOG2_E = math.log2(math.e)
LANES = 128
F32 = jnp.float32
BF16 = jnp.bfloat16
AXES = ("group", "tile")
PARAMS = pltpu.CompilerParams(vmem_limit_bytes=24 * 1024 * 1024)


def dot(left, right, left_dim, right_dim, precision=None):
    return lax.dot_general(
        left,
        right,
        (((left_dim,), (right_dim,)), ((), ())),
        preferred_element_type=F32,
        precision=precision,
    )


def iota(shape, dim):
    return lax.broadcasted_iota(jnp.int32, shape, dim)


def shift_rows(values, amounts, right):
    width = values.shape[1]
    for bit in range(4):
        step = 1 << bit
        moved = pltpu.roll(values, step if right else width - step, 1)
        values = jnp.where((amounts & step) != 0, moved, values)
    return values


def bias_kernel(heads, windows, table_ref, out_ref, pad_ref):
    span = 2 * WIN * WIN
    tokens = WIN * WIN
    offsets = 2 * WIN - 1
    block = offsets + 1
    pad_ref[...] = jnp.zeros_like(pad_ref)
    for head in range(heads):
        pad_ref[head * block : head * block + offsets, :offsets] = table_ref[:, head, :]
    padded = pad_ref[...]
    parts = []
    for _ in range(3):
        part = padded.astype(BF16)
        parts.append(part)
        padded = padded - part.astype(F32)
    chosen = iota((LANES, span), 1) % 32 == offsets - 1 - iota((LANES, span), 0)
    spread = dot(jnp.concatenate(parts, 0), jnp.where(chosen, 1.0, 0.0).astype(BF16), 1, 0)
    size = heads * block
    spread = spread[:size] + spread[size : 2 * size] + spread[2 * size :]
    flats = []
    for odd in range(2):
        wanted = offsets - 1 - iota((block, span), 0)
        keep = (iota((block, span), 1) // 32) * 2 + odd == wanted
        for head in range(heads):
            mine = spread[head * block : (head + 1) * block]
            flat = jnp.sum(jnp.where(keep, mine, 0.0), axis=0, keepdims=True)
            flats.append(jnp.broadcast_to(flat, (WIN, span)))
    rows = heads * WIN
    amounts = WIN - 1 - iota((rows, span), 0) % WIN
    even = shift_rows(jnp.concatenate(flats[:heads], 0), amounts, False)
    odd = shift_rows(jnp.concatenate(flats[heads:], 0), amounts, False)
    odd = pltpu.roll(odd, WIN, 1)
    strip = jnp.where(iota((rows, span), 1) % 32 < WIN, even, odd) * LOG2_E
    last_row = (lax.axis_index("group") == 0).astype(jnp.int32)
    last_col = (lax.axis_index("tile") == 0).astype(jnp.int32)
    key = iota((WIN, tokens), 1)
    query_x = iota((WIN, tokens), 0)
    key_low = (key >= tokens // 2).astype(jnp.int32)
    cross_col = ((key % WIN >= SHIFT) != (query_x >= SHIFT)).astype(jnp.int32)
    for fine in range(8):
        moved = pltpu.roll(strip, (span - WIN * fine) % span, 1)
        for coarse in range(2):
            y = WIN - 1 - (8 * coarse + fine)
            cross_row = key_low if y < SHIFT else 1 - key_low
            for window in range(windows):
                apart = cross_row * last_row
                if window == windows - 1:
                    apart = apart + cross_col * last_col
                extra = jnp.where(apart > 0, -1e30, 0.0)
                for head in range(heads):
                    part = moved[
                        head * WIN : (head + 1) * WIN,
                        LANES * coarse : LANES * coarse + tokens,
                    ]
                    start = head * tokens + y * WIN
                    out_ref[window, start : start + WIN, :] = part + extra


def mean_of(values):
    return jnp.mean(values, axis=-1, keepdims=True)


def norm(values):
    centred = values - mean_of(values)
    scale = lax.rsqrt(mean_of(centred * centred) + NORM_EPS)
    return centred * scale, scale


def norm_back(grad, unit, scale):
    return scale * (grad - mean_of(grad) - unit * mean_of(grad * unit))


def cut_kernel(token_ref, cot_ref, table_ref, below_ref, right_ref, diag_ref, table_out, sems):
    copies = []

    def copy(source, target):
        copies.append(pltpu.make_async_copy(source, target, sems.at[len(copies)]))

    keep = token_ref.shape[1] - SHIFT
    high, low = pl.ds(0, SHIFT), pl.ds(SHIFT, SHIFT)
    most, rest = pl.ds(0, keep), pl.ds(keep, SHIFT)
    for index, tile_ref in enumerate((token_ref, cot_ref)):
        copy(tile_ref.at[low, most], below_ref.at[index])
        copy(tile_ref.at[high, rest], right_ref.at[index])
        copy(tile_ref.at[low, rest], diag_ref.at[index])
    copy(table_ref, table_out)
    for each in copies:
        each.start()
    for each in copies:
        each.wait()


def block_kernel(heads, first, count, last, *refs):
    token_ref, cot_ref, below_ref = refs[:3]
    refs = refs[3:]
    if last:
        right_ref, diag_ref, sums_in, strip_in, gains_in = refs[:5]
        refs = refs[5:]
    bias_ref, gain1_ref, qkv_ref, proj_ref, gain2_ref, fc1_ref, fc2_ref = refs[:7]
    own_out, below_out = refs[7:9]
    refs = refs[9:]
    if last:
        right_out, diag_out, keep_out, send_out, grads_ref = refs[:5]
        refs = refs[5:]
    else:
        sums_out, strip_out, gains_out = refs[:3]
        refs = refs[3:]
    x_ref, c_ref, n_ref, unit_ref, scale_ref, q_ref, k_ref, v_ref = refs[:8]
    p_ref, att_ref, out_f32_ref, inverse_ref, dh_ref, dqkv_ref, ds_ref, dsn_ref = refs[8:16]
    inner_ref, before_ref, out_ref = refs[16:]

    tokens = WIN * WIN
    width = token_ref.shape[2]
    head_size = width // heads
    hidden_units = fc1_ref.shape[1]

    def put(row, value):
        rows = slice(row, row + value.shape[0])
        if last:
            grads_ref[rows, :] = (sums_in[rows, :] + value).astype(BF16)
        else:
            sums_out[rows, :] = value

    def assemble(tile_ref, index, target):
        tile = tile_ref[...].astype(F32)
        above = below_ref[index].astype(F32)
        for window in range(count):
            cols = slice(WIN * (first + window) + SHIFT, WIN * (first + window) + SHIFT + WIN)
            if last and window == count - 1:
                left = right_ref[index].astype(F32)
                diag = diag_ref[index].astype(F32)
                top = jnp.concatenate([diag, above[:, :SHIFT]], 1)
                low = jnp.concatenate([left, tile[:SHIFT, :SHIFT]], 1)
            else:
                top = above[:, cols]
                low = tile[:SHIFT, cols]
            both = jnp.concatenate([top, low], 0).reshape(tokens, width)
            target[window * tokens : (window + 1) * tokens, :] = both.astype(target.dtype)

    assemble(token_ref, 0, x_ref)
    assemble(cot_ref, 1, c_ref)

    unit1, scale1 = norm(x_ref[...])
    unit_ref[...] = unit1
    scale_ref[...] = scale1
    normed = (unit1 * gain1_ref[...]).astype(BF16)
    n_ref[...] = normed
    projected = dot(normed, qkv_ref[...], 1, 0)
    q_ref[...] = projected[:, :width]
    k_ref[...] = projected[:, width : 2 * width].astype(BF16)
    v_ref[...] = projected[:, 2 * width :].astype(BF16)
    lane_head = iota((1, width), 1) // head_size
    score_scale = head_size ** (-0.5)

    def of_head(values, head):
        return jnp.where(lane_head == head, values, 0.0).astype(BF16)

    for window in range(count):
        span = slice(window * tokens, (window + 1) * tokens)
        query = q_ref[span, :]
        keys = k_ref[span, :]
        value = v_ref[span, :].astype(F32)
        sources = []
        for head in range(heads):
            scores = dot(of_head(query, head), keys, 1, 1) * (score_scale * LOG2_E)
            scores = scores + bias_ref[first + window, head * tokens : (head + 1) * tokens, :]
            weights = jnp.exp2(scores - jnp.max(scores, axis=-1, keepdims=True))
            p_ref[window, :, head * tokens : (head + 1) * tokens] = weights.astype(BF16)
            ones = jnp.broadcast_to(of_head(jnp.ones((1, width), F32), head), (tokens, width))
            sources.append(jnp.concatenate([of_head(value, head), ones], 1))
        both = dot(p_ref[window], jnp.concatenate(sources, 0), 1, 0)
        inverse = 1.0 / both[:, width:]
        attended = both[:, :width] * inverse
        inverse_ref[span, :] = inverse
        out_f32_ref[span, :] = attended
        att_ref[span, :] = attended.astype(BF16)

    hidden = x_ref[...] + dot(att_ref[...], proj_ref[...], 1, 0).astype(BF16).astype(F32)
    unit2, scale2 = norm(hidden)
    normed2 = (unit2 * gain2_ref[...]).astype(BF16)
    cot = c_ref[...]
    root = math.sqrt(0.5)
    step = 2 * width
    for part in range(hidden_units // step):
        cols = slice(part * step, (part + 1) * step)
        before = dot(normed2, fc1_ref[:, cols], 1, 0)
        normal = 0.5 * (1.0 + lax.erf(before * root))
        inner_ref[:, cols] = (before * normal).astype(BF16)
        density = jnp.exp2(before * before * (-0.5 * LOG2_E)) * (1.0 / math.sqrt(2.0 * math.pi))
        slope = normal + before * density
        grad_inner = dot(cot, fc2_ref[cols, :], 1, 1).astype(BF16).astype(F32)
        before_ref[:, cols] = (grad_inner * slope).astype(BF16)
    inner = inner_ref[...]
    grad_before = before_ref[...]
    out_ref[...] = hidden + dot(inner, fc2_ref[...], 1, 0)
    back = dot(grad_before, fc1_ref[...], 1, 1).astype(BF16).astype(F32)
    grad_fc1 = dot(normed2, grad_before, 0, 0)
    for part in range(hidden_units // width):
        put(part * width, grad_fc1[:, part * width : (part + 1) * width])
    put(hidden_units, dot(inner, cot, 0, 0))
    grad_gain2 = jnp.sum(back * unit2, axis=0, keepdims=True)
    grad_hidden = cot.astype(F32) + norm_back(back * gain2_ref[...], unit2, scale2)
    dh_ref[...] = grad_hidden

    grad_attended = grad_hidden.astype(BF16)
    put(2 * hidden_units + 3 * width, dot(att_ref[...], grad_attended, 0, 0))
    grad_heads = dot(grad_attended, proj_ref[...], 1, 1).astype(BF16).astype(F32)

    minus = jnp.full((tokens, width), -1.0, BF16)
    for window in range(count):
        span = slice(window * tokens, (window + 1) * tokens)
        query = q_ref[span, :]
        keys = k_ref[span, :].astype(F32)
        value = jnp.concatenate([v_ref[span, :], minus], 1)
        scaled = (grad_heads[span, :] * inverse_ref[span, :]).astype(BF16).astype(F32)
        inside = scaled * out_f32_ref[span, :]
        inside_high = inside.astype(BF16).astype(F32)
        inside_low = pltpu.roll(inside - inside_high, head_size, 1)
        query_t = query.T.astype(BF16)
        scaled_t = scaled.T.astype(BF16)
        grad_k, grad_v, sources = [], [], []
        for head in range(heads):
            rows = slice(head * tokens, (head + 1) * tokens)
            part = slice(head * head_size, (head + 1) * head_size)
            extra = jnp.where(
                lane_head == head,
                inside_high,
                jnp.where(lane_head == (head + 1) % heads, inside_low, 0.0),
            ).astype(BF16)
            grad_weights = dot(jnp.concatenate([of_head(scaled, head), extra], 1), value, 1, 1)
            weights = p_ref[window, :, rows]
            grad_scores = grad_weights * weights.astype(F32)
            if window == 0:
                ds_ref[rows, :] = grad_scores
            else:
                ds_ref[rows, :] += grad_scores
            narrow = grad_scores.astype(BF16)
            dsn_ref[:, rows] = narrow
            sources.append(of_head(keys, head))
            grad_k.append(dot(query_t[part, :], narrow, 1, 0))
            grad_v.append(dot(scaled_t[part, :], weights, 1, 0))
        grad_q = dot(dsn_ref[...], jnp.concatenate(sources, 0), 1, 0)
        dqkv_ref[span, :width] = (grad_q * score_scale).astype(BF16)
        grad_k = jnp.concatenate(grad_k, 0).T
        dqkv_ref[span, width : 2 * width] = (grad_k * score_scale).astype(BF16)
        dqkv_ref[span, 2 * width :] = jnp.concatenate(grad_v, 0).T.astype(BF16)

    grad_projected = dqkv_ref[...]
    grad_qkv = dot(n_ref[...], grad_projected, 0, 0)
    for part in range(3):
        put(2 * hidden_units + part * width, grad_qkv[:, part * width : (part + 1) * width])
    grad_normed = dot(grad_projected, qkv_ref[...], 1, 1).astype(BF16).astype(F32)
    unit1 = unit_ref[...]
    grad_gain1 = jnp.sum(grad_normed * unit1, axis=0, keepdims=True)
    grad_x = dh_ref[...] + norm_back(grad_normed * gain1_ref[...], unit1, scale_ref[...])
    gains = jnp.concatenate([grad_gain1, grad_gain2, jnp.zeros((6, width), F32)], 0)

    lanes = 2 * tokens
    rows = heads * WIN
    blank = jnp.zeros((WIN, LANES), F32)
    strip = strip_in[...] if last else jnp.zeros((rows, lanes), F32)
    for fine in range(8):
        near, far = WIN - 1 - fine, WIN - 9 - fine
        blocks = []
        for head in range(heads):
            above = ds_ref[head * tokens + near * WIN : head * tokens + (near + 1) * WIN, :]
            under = ds_ref[head * tokens + far * WIN : head * tokens + (far + 1) * WIN, :]
            blocks.append(
                jnp.concatenate([above, blank, blank], 1) + jnp.concatenate([blank, under, blank], 1)
            )
        block = jnp.concatenate(blocks, 0)
        strip = strip + (pltpu.roll(block, WIN * fine, 1) if fine else block)

    if last:
        finish_table(heads, strip, grads_ref, 2 * hidden_units + 4 * width)
        row = 2 * hidden_units + 4 * width + heads * 2 * WIN
        blank = jnp.zeros((grads_ref.shape[0] - row - 8, width), F32)
        grads_ref[row:, :] = jnp.concatenate([gains_in[...] + gains, blank], 0).astype(BF16)
        half = keep_out.shape[0]
        core = lax.axis_index("group") % 2
        keep_out[...] = grads_ref[pl.ds(pl.multiple_of(core * half, 16), half), :]
        send_out[...] = grads_ref[pl.ds(pl.multiple_of((1 - core) * half, 16), half), :]
    else:
        strip_out[...] = strip
        gains_out[...] = gains

    for index, values in enumerate((out_ref[...], grad_x)):
        for window in range(count):
            start = WIN * window
            block = values[window * tokens : (window + 1) * tokens, :].reshape(WIN, WIN, width)
            top, low = block[:SHIFT], block[SHIFT:]
            if last and window == count - 1:
                own_out[index, :, start:, :] = low[:, SHIFT:].astype(BF16)
                below_out[index, :, start:, :] = top[:, SHIFT:].astype(BF16)
                right_out[index] = low[:, :SHIFT].astype(BF16)
                diag_out[index] = top[:, :SHIFT].astype(BF16)
            else:
                own_out[index, :, start : start + WIN, :] = low.astype(BF16)
                below_out[index, :, start : start + WIN, :] = top.astype(BF16)


def finish_table(heads, strip, grads_ref, row):
    rows, lanes = strip.shape
    lane = iota((rows, lanes), 1)
    amounts = WIN - 1 - iota((rows, lanes), 0) % WIN
    offsets = 2 * WIN
    table = jnp.zeros((heads * offsets, LANES), F32)
    for odd in range(2):
        chosen = jnp.where((lane // WIN) % 2 == odd, strip, 0.0)
        if odd:
            chosen = pltpu.roll(chosen, lanes - WIN, 1)
        chosen = shift_rows(chosen, amounts, True)
        wanted = offsets - 2 - iota((offsets, lanes), 0)
        where_row = (iota((offsets, lanes), 1) // 32) * 2 + odd == wanted
        terms = []
        for head in range(heads):
            flat = jnp.sum(chosen[head * WIN : (head + 1) * WIN, :], axis=0, keepdims=True)
            terms.append(jnp.where(where_row, flat, 0.0))
        terms = jnp.concatenate(terms, 0).astype(BF16)
        pick_lane = iota((lanes, LANES), 0) % 32
        pick = jnp.where(pick_lane == offsets - 2 - iota((lanes, LANES), 1), 1.0, 0.0).astype(BF16)
        table = table + dot(terms, pick, 1, 0)
    grads_ref[row : row + heads * offsets, :] = table.astype(BF16)


def pair_kernel(first_ref, second_ref, out_ref):
    total = first_ref[...].astype(F32) + second_ref[...].astype(F32)
    out_ref[...] = total.astype(out_ref.dtype)


def sum_kernel(in_ref, out_ref):
    total = in_ref[0].astype(F32)
    for index in range(1, in_ref.shape[0]):
        total = total + in_ref[index].astype(F32)
    total = total.astype(out_ref.dtype)
    for index in range(out_ref.shape[0]):
        out_ref[index] = total


def unpack_kernel(
    heads,
    factor,
    mine_ref,
    other_ref,
    diag_ref,
    above_first_ref,
    above_last_ref,
    left_ref,
    own_first_ref,
    own_last_ref,
    out_ref,
    grad_ref,
    gain1_ref,
    qkv_ref,
    proj_ref,
    table_ref,
    gain2_ref,
    fc1_ref,
    fc2_ref,
    summed_ref,
):
    width, hidden_units = fc1_ref.shape
    half = mine_ref.shape[0]
    early = own_first_ref.shape[2]
    for index, target in enumerate((out_ref, grad_ref)):
        target[:SHIFT, :SHIFT, :] = own_last_ref[index]
        target[:SHIFT, SHIFT : SHIFT + early, :] = own_first_ref[index]
        target[:SHIFT, SHIFT + early :, :] = left_ref[index]
        target[SHIFT:, :SHIFT, :] = above_last_ref[index]
        target[SHIFT:, SHIFT : SHIFT + early, :] = above_first_ref[index]
        target[SHIFT:, SHIFT + early :, :] = diag_ref[index]
    core = lax.axis_index("group") % 2
    summed_ref[pl.ds(pl.multiple_of(core * half, 16), half), :] = mine_ref[...]
    summed_ref[pl.ds(pl.multiple_of((1 - core) * half, 16), half), :] = other_ref[...]
    offsets = 2 * WIN

    def rows(start, count):
        return summed_ref[start : start + count, :].astype(F32) * factor

    for part in range(hidden_units // width):
        fc1_ref[:, part * width : (part + 1) * width] = rows(part * width, width)
    fc2_ref[...] = rows(hidden_units, hidden_units)
    for part in range(3):
        qkv_ref[:, part * width : (part + 1) * width] = rows(2 * hidden_units + part * width, width)
    start = 2 * hidden_units + 3 * width
    proj_ref[...] = rows(start, width)
    start = start + width
    for head in range(heads):
        block = rows(start + head * offsets, offsets)
        table_ref[:, head, :] = block[: offsets - 1, : offsets - 1]
    start = start + heads * offsets
    gains = rows(start, 16)
    gain1_ref[...] = gains[0:1]
    gain2_ref[...] = gains[1:2]


def neighbour_pairs(row_step, col_step):
    groups, tiles = lax.axis_size("group"), lax.axis_size("tile")
    pairs = []
    for group in range(groups):
        for tile in range(tiles):
            target = ((group + row_step) % groups) * tiles + (tile + col_step) % tiles
            pairs.append((group * tiles + tile, target))
    return pairs


def passed_along(value, row_step, col_step):
    return lax.ppermute(value, AXES, neighbour_pairs(row_step, col_step))


def shards(tokens, gain1, w_qkv, w_proj, bias_table, gain2, w_fc1, w_fc2, cotangent):
    row_count, col_count, width = tokens.shape
    heads = bias_table.shape[0]
    hidden_units = w_fc1.shape[1]
    groups, tiles = lax.axis_size("group"), lax.axis_size("tile")
    devices = groups * tiles
    windows = col_count // WIN
    token_count = WIN * WIN
    keep = col_count - SHIFT

    vmem = pl.BlockSpec(memory_space=pltpu.VMEM)

    def array(shape, dtype=BF16):
        return jax.ShapeDtypeStruct(shape, dtype)

    table = bias_table.transpose(1, 0, 2)
    hbm = pl.BlockSpec(memory_space=pltpu.HBM)
    below, right, diag, table = pl.pallas_call(
        cut_kernel,
        out_shape=(
            array((2, SHIFT, keep, width)),
            array((2, SHIFT, SHIFT, width)),
            array((2, SHIFT, SHIFT, width)),
            array(table.shape, F32),
        ),
        in_specs=[hbm] * 3,
        out_specs=(vmem,) * 4,
        scratch_shapes=[pltpu.SemaphoreType.DMA((7,))],
        name="cut",
        compiler_params=PARAMS,
    )(*(pltpu.with_memory_space_constraint(each, pltpu.HBM) for each in (tokens, cotangent, table)))
    below = passed_along(below, 1, 0)
    right = passed_along(right, 0, 1)
    diag = passed_along(diag, 1, 1)

    bias = pl.pallas_call(
        functools.partial(bias_kernel, heads, windows),
        out_shape=jax.ShapeDtypeStruct((windows, heads * token_count, token_count), F32),
        in_specs=[vmem],
        out_specs=vmem,
        scratch_shapes=[pltpu.VMEM((heads * 2 * WIN, LANES), F32)],
        name="bias",
        compiler_params=PARAMS,
        cost_estimate=pl.CostEstimate(flops=8_000_000, bytes_accessed=2_000_000, transcendentals=0),
    )(table)

    used = 2 * hidden_units + 4 * width + heads * 2 * WIN + 16
    members = devices // 2
    chunk = (used + devices * 8 - 1) // (devices * 8) * 8
    half = chunk * members
    weights = (gain1.reshape(1, width), w_qkv, w_proj, gain2.reshape(1, width), w_fc1, w_fc2)
    sum_rows = 2 * hidden_units + 4 * width

    def block(first, count, last, inputs, outputs):
        total = count * token_count
        scratch = [
            pltpu.VMEM((total, width), F32),
            pltpu.VMEM((total, width), BF16),
            pltpu.VMEM((total, width), BF16),
            pltpu.VMEM((total, width), F32),
            pltpu.VMEM((total, 1), F32),
            pltpu.VMEM((total, width), F32),
            pltpu.VMEM((total, width), BF16),
            pltpu.VMEM((total, width), BF16),
            pltpu.VMEM((count, token_count, heads * token_count), BF16),
            pltpu.VMEM((total, width), BF16),
            pltpu.VMEM((total, width), F32),
            pltpu.VMEM((total, width), F32),
            pltpu.VMEM((total, width), F32),
            pltpu.VMEM((total, 3 * width), BF16),
            pltpu.VMEM((heads * token_count, token_count), F32),
            pltpu.VMEM((token_count, heads * token_count), BF16),
            pltpu.VMEM((total, hidden_units), BF16),
            pltpu.VMEM((total, hidden_units), BF16),
            pltpu.VMEM((total, width), F32),
        ]
        if last:
            scratch = [pltpu.VMEM((2 * half, width), BF16)] + scratch
        inputs = inputs + (bias,) + weights
        return pl.pallas_call(
            functools.partial(block_kernel, heads, first, count, last),
            out_shape=outputs,
            in_specs=[vmem] * len(inputs),
            out_specs=(vmem,) * len(outputs),
            scratch_shapes=scratch,
            name="last" if last else "first",
            compiler_params=PARAMS,
            cost_estimate=pl.CostEstimate(
                flops=1_000_000_000 * count, bytes_accessed=2_000_000, transcendentals=1_000_000
            ),
        )(*inputs)

    early = WIN * (windows - 1)
    own_first, below_first, sums, strip, gains = block(
        0,
        windows - 1,
        False,
        (tokens, cotangent, below),
        (
            array((2, SHIFT, early, width)),
            array((2, SHIFT, early, width)),
            array((sum_rows, width), F32),
            array((heads * WIN, 2 * token_count), F32),
            array((8, width), F32),
        ),
    )
    back_first = passed_along(below_first, -1, 0)
    own_last, below_last, right_last, diag_last, kept, sent = block(
        windows - 1,
        1,
        True,
        (tokens, cotangent, below, right, diag, sums, strip, gains),
        (
            array((2, SHIFT, SHIFT, width)),
            array((2, SHIFT, SHIFT, width)),
            array((2, SHIFT, SHIFT, width)),
            array((2, SHIFT, SHIFT, width)),
            array((half, width)),
            array((half, width)),
        ),
    )
    back_right = passed_along(right_last, 0, -1)
    back_diag = passed_along(diag_last, -1, -1)
    back_below = passed_along(below_last, -1, 0)

    pairs = [(index, index + tiles if index // tiles % 2 == 0 else index - tiles) for index in range(devices)]
    same_core = [
        [index for index in range(devices) if index // tiles % 2 == core] for core in range(2)
    ]

    def exchanged(value):
        return lax.all_to_all(value, AXES, 0, 0, tiled=True, axis_index_groups=same_core)

    received = lax.ppermute(sent, AXES, pairs)
    paired = pl.pallas_call(
        pair_kernel,
        out_shape=jax.ShapeDtypeStruct((half, width), BF16),
        in_specs=[vmem] * 2,
        out_specs=vmem,
        name="pair",
        compiler_params=PARAMS,
    )(kept, received)
    copies = pl.pallas_call(
        sum_kernel,
        out_shape=jax.ShapeDtypeStruct((members, chunk, width), BF16),
        in_specs=[vmem],
        out_specs=vmem,
        name="add",
        compiler_params=PARAMS,
    )(exchanged(paired.reshape(members, chunk, width)))
    mine = exchanged(copies).reshape(half, width)
    other = lax.ppermute(mine, AXES, pairs)

    factor = 1.0 / math.sqrt(row_count * groups * col_count * tiles)
    (
        block_output,
        grad_tokens,
        grad_gain1,
        grad_qkv,
        grad_proj,
        grad_table,
        grad_gain2,
        grad_fc1,
        grad_fc2,
    ) = pl.pallas_call(
        functools.partial(unpack_kernel, heads, factor),
        out_shape=(
            array(tokens.shape),
            array(tokens.shape),
            jax.ShapeDtypeStruct((1, width), F32),
            jax.ShapeDtypeStruct(w_qkv.shape, F32),
            jax.ShapeDtypeStruct(w_proj.shape, F32),
            jax.ShapeDtypeStruct((bias_table.shape[1], heads, bias_table.shape[2]), F32),
            jax.ShapeDtypeStruct((1, width), F32),
            jax.ShapeDtypeStruct(w_fc1.shape, F32),
            jax.ShapeDtypeStruct(w_fc2.shape, F32),
        ),
        in_specs=[vmem] * 8,
        out_specs=(vmem,) * 9,
        scratch_shapes=[pltpu.VMEM((2 * half, width), BF16)],
        name="unpack",
        compiler_params=PARAMS,
    )(mine, other, back_diag, back_first, back_below, back_right, own_first, own_last)

    return (
        block_output,
        grad_tokens,
        grad_gain1.reshape(width),
        grad_qkv,
        grad_proj,
        grad_table.transpose(1, 0, 2),
        grad_gain2.reshape(width),
        grad_fc1,
        grad_fc2,
    )


def solution(mesh):
    tile_spec = P("group", "tile", None)
    return jax.shard_map(
        shards,
        mesh=mesh,
        in_specs=(tile_spec, P(), P(), P(), P(), P(), P(), P(), tile_spec),
        out_specs=(tile_spec, tile_spec, P(), P(), P(), P(), P(), P(), P()),
        check_vma=False,
    )
```

```python
import functools
import math

import jax
import jax.numpy as jnp
from jax import lax
from jax.experimental import pallas as pl
from jax.experimental.pallas import tpu as pltpu
from jax.sharding import PartitionSpec as P


WIN = 16
SHIFT = 8
NORM_EPS = 1e-05
LOG2_E = math.log2(math.e)
LANES = 128
F32 = jnp.float32
BF16 = jnp.bfloat16
AXES = ("group", "tile")
PARAMS = pltpu.CompilerParams(vmem_limit_bytes=24 * 1024 * 1024)


def dot(left, right, left_dim, right_dim, precision=None):
    return lax.dot_general(
        left,
        right,
        (((left_dim,), (right_dim,)), ((), ())),
        preferred_element_type=F32,
        precision=precision,
    )


def iota(shape, dim):
    return lax.broadcasted_iota(jnp.int32, shape, dim)


def shift_rows(values, amounts, right):
    width = values.shape[1]
    for bit in range(4):
        step = 1 << bit
        moved = pltpu.roll(values, step if right else width - step, 1)
        values = jnp.where((amounts & step) != 0, moved, values)
    return values


def bias_kernel(heads, windows, table_ref, out_ref, pad_ref):
    span = 2 * WIN * WIN
    tokens = WIN * WIN
    offsets = 2 * WIN - 1
    block = offsets + 1
    pad_ref[...] = jnp.zeros_like(pad_ref)
    for head in range(heads):
        pad_ref[head * block : head * block + offsets, :offsets] = table_ref[:, head, :]
    padded = pad_ref[...]
    parts = []
    for _ in range(3):
        part = padded.astype(BF16)
        parts.append(part)
        padded = padded - part.astype(F32)
    chosen = iota((LANES, span), 1) % 32 == offsets - 1 - iota((LANES, span), 0)
    spread = dot(jnp.concatenate(parts, 0), jnp.where(chosen, 1.0, 0.0).astype(BF16), 1, 0)
    size = heads * block
    spread = spread[:size] + spread[size : 2 * size] + spread[2 * size :]
    flats = []
    for odd in range(2):
        wanted = offsets - 1 - iota((block, span), 0)
        keep = (iota((block, span), 1) // 32) * 2 + odd == wanted
        for head in range(heads):
            mine = spread[head * block : (head + 1) * block]
            flat = jnp.sum(jnp.where(keep, mine, 0.0), axis=0, keepdims=True)
            flats.append(jnp.broadcast_to(flat, (WIN, span)))
    rows = heads * WIN
    amounts = WIN - 1 - iota((rows, span), 0) % WIN
    even = shift_rows(jnp.concatenate(flats[:heads], 0), amounts, False)
    odd = shift_rows(jnp.concatenate(flats[heads:], 0), amounts, False)
    odd = pltpu.roll(odd, WIN, 1)
    strip = jnp.where(iota((rows, span), 1) % 32 < WIN, even, odd) * LOG2_E
    last_row = (lax.axis_index("group") == 0).astype(jnp.int32)
    last_col = (lax.axis_index("tile") == 0).astype(jnp.int32)
    key = iota((WIN, tokens), 1)
    query_x = iota((WIN, tokens), 0)
    key_low = (key >= tokens // 2).astype(jnp.int32)
    cross_col = ((key % WIN >= SHIFT) != (query_x >= SHIFT)).astype(jnp.int32)
    for fine in range(8):
        moved = pltpu.roll(strip, (span - WIN * fine) % span, 1)
        for coarse in range(2):
            y = WIN - 1 - (8 * coarse + fine)
            cross_row = key_low if y < SHIFT else 1 - key_low
            for window in range(windows):
                apart = cross_row * last_row
                if window == windows - 1:
                    apart = apart + cross_col * last_col
                extra = jnp.where(apart > 0, -1e30, 0.0)
                for head in range(heads):
                    part = moved[
                        head * WIN : (head + 1) * WIN,
                        LANES * coarse : LANES * coarse + tokens,
                    ]
                    start = head * tokens + y * WIN
                    out_ref[window, start : start + WIN, :] = part + extra


def mean_of(values):
    return jnp.mean(values, axis=-1, keepdims=True)


def norm(values):
    centred = values - mean_of(values)
    scale = lax.rsqrt(mean_of(centred * centred) + NORM_EPS)
    return centred * scale, scale


def norm_back(grad, unit, scale):
    return scale * (grad - mean_of(grad) - unit * mean_of(grad * unit))


def cut_kernel(token_ref, cot_ref, table_ref, below_ref, right_ref, diag_ref, table_out, sems):
    copies = []

    def copy(source, target):
        copies.append(pltpu.make_async_copy(source, target, sems.at[len(copies)]))

    keep = token_ref.shape[1] - SHIFT
    high, low = pl.ds(0, SHIFT), pl.ds(SHIFT, SHIFT)
    most, rest = pl.ds(0, keep), pl.ds(keep, SHIFT)
    for index, tile_ref in enumerate((token_ref, cot_ref)):
        copy(tile_ref.at[low, most], below_ref.at[index])
        copy(tile_ref.at[high, rest], right_ref.at[index])
        copy(tile_ref.at[low, rest], diag_ref.at[index])
    copy(table_ref, table_out)
    for each in copies:
        each.start()
    for each in copies:
        each.wait()


STATE = ("x", "n", "unit", "scale", "q", "k", "v", "p", "att", "out", "inverse")


def assemble(tile_ref, piece_refs, index, window, windows):
    tile = tile_ref[...].astype(F32)
    above = piece_refs[0][index].astype(F32)
    cols = slice(WIN * window + SHIFT, WIN * window + SHIFT + WIN)
    if window == windows - 1:
        left = piece_refs[1][index].astype(F32)
        diag = piece_refs[2][index].astype(F32)
        top = jnp.concatenate([diag, above[:, :SHIFT]], 1)
        low = jnp.concatenate([left, tile[:SHIFT, :SHIFT]], 1)
    else:
        top = above[:, cols]
        low = tile[:SHIFT, cols]
    return jnp.concatenate([top, low], 0).reshape(WIN * WIN, tile.shape[2])


def of_head(values, head, head_size):
    lane_head = iota((1, values.shape[1]), 1) // head_size
    return jnp.where(lane_head == head, values, 0.0).astype(BF16)


def attend(heads, window, bias_ref, gain1_ref, qkv_ref, state):
    tokens, width = state["x"].shape
    head_size = width // heads
    unit, scale = norm(state["x"][...])
    state["unit"][...] = unit
    state["scale"][...] = scale
    normed = (unit * gain1_ref[...]).astype(BF16)
    state["n"][...] = normed
    projected = dot(normed, qkv_ref[...], 1, 0)
    state["q"][...] = projected[:, :width]
    state["k"][...] = projected[:, width : 2 * width].astype(BF16)
    state["v"][...] = projected[:, 2 * width :].astype(BF16)
    query = state["q"][...]
    keys = state["k"][...]
    value = state["v"][...].astype(F32)
    sources = []
    for head in range(heads):
        rows = slice(head * tokens, (head + 1) * tokens)
        scores = dot(of_head(query, head, head_size), keys, 1, 1) * (head_size ** (-0.5) * LOG2_E)
        scores = scores + bias_ref[window, rows, :]
        weights = jnp.exp2(scores - jnp.max(scores, axis=-1, keepdims=True))
        state["p"][:, rows] = weights.astype(BF16)
        ones = jnp.broadcast_to(of_head(jnp.ones((1, width), F32), head, head_size), (tokens, width))
        sources.append(jnp.concatenate([of_head(value, head, head_size), ones], 1))
    both = dot(state["p"][...], jnp.concatenate(sources, 0), 1, 0)
    inverse = 1.0 / both[:, width:]
    attended = both[:, :width] * inverse
    state["inverse"][...] = inverse
    state["out"][...] = attended
    state["att"][...] = attended.astype(BF16)


def early_kernel(heads, windows, token_ref, below_ref, bias_ref, gain1_ref, qkv_ref, *refs):
    for window in range(windows - 1):
        state = dict(zip(STATE, refs[window * len(STATE) : (window + 1) * len(STATE)]))
        state["x"][...] = assemble(token_ref, (below_ref,), 0, window, windows)
        attend(heads, window, bias_ref, gain1_ref, qkv_ref, state)


def block_kernel(heads, windows, *refs):
    token_ref, cot_ref, below_ref, right_ref, diag_ref = refs[:5]
    bias_ref, gain1_ref, qkv_ref, proj_ref, gain2_ref, fc1_ref, fc2_ref = refs[5:12]
    refs = refs[12:]
    states = []
    for _ in range(windows - 1):
        states.append(dict(zip(STATE, refs)))
        refs = refs[len(STATE) :]
    own_out, below_out, right_out, diag_out, keep_out, send_out = refs[:6]
    grads_ref, c_ref, dqkv_ref, ds_ref, dsn_ref, inner_ref, before_ref, out_ref = refs[6:14]
    states.append(dict(zip(STATE, refs[14:])))
    count = windows

    tokens = WIN * WIN
    width = token_ref.shape[2]
    head_size = width // heads
    hidden_units = fc1_ref.shape[1]
    score_scale = head_size ** (-0.5)
    lane_head = iota((1, width), 1) // head_size
    pieces = (below_ref, right_ref, diag_ref)

    def put(row, value):
        grads_ref[row : row + value.shape[0], :] = value.astype(BF16)

    def stacked(name):
        return jnp.concatenate([state[name][...] for state in states], 0)

    states[-1]["x"][...] = assemble(token_ref, pieces, 0, windows - 1, windows)
    for window in range(windows):
        piece = assemble(cot_ref, pieces, 1, window, windows)
        c_ref[window * tokens : (window + 1) * tokens, :] = piece.astype(BF16)
    attend(heads, windows - 1, bias_ref, gain1_ref, qkv_ref, states[-1])

    attended = stacked("att")
    hidden = stacked("x") + dot(attended, proj_ref[...], 1, 0).astype(BF16).astype(F32)
    unit2, scale2 = norm(hidden)
    normed2 = (unit2 * gain2_ref[...]).astype(BF16)
    cot = c_ref[...]
    root = math.sqrt(0.5)
    step = 2 * width
    for part in range(hidden_units // step):
        cols = slice(part * step, (part + 1) * step)
        before = dot(normed2, fc1_ref[:, cols], 1, 0)
        normal = 0.5 * (1.0 + lax.erf(before * root))
        inner_ref[:, cols] = (before * normal).astype(BF16)
        density = jnp.exp2(before * before * (-0.5 * LOG2_E)) * (1.0 / math.sqrt(2.0 * math.pi))
        slope = normal + before * density
        grad_inner = dot(cot, fc2_ref[cols, :], 1, 1).astype(BF16).astype(F32)
        before_ref[:, cols] = (grad_inner * slope).astype(BF16)
    inner = inner_ref[...]
    grad_before = before_ref[...]
    out_ref[...] = hidden + dot(inner, fc2_ref[...], 1, 0)
    back = dot(grad_before, fc1_ref[...], 1, 1).astype(BF16).astype(F32)
    grad_fc1 = dot(normed2, grad_before, 0, 0)
    for part in range(hidden_units // width):
        put(part * width, grad_fc1[:, part * width : (part + 1) * width])
    put(hidden_units, dot(inner, cot, 0, 0))
    grad_gain2 = jnp.sum(back * unit2, axis=0, keepdims=True)
    grad_hidden = cot.astype(F32) + norm_back(back * gain2_ref[...], unit2, scale2)

    grad_attended = grad_hidden.astype(BF16)
    put(2 * hidden_units + 3 * width, dot(attended, grad_attended, 0, 0))
    grad_heads = dot(grad_attended, proj_ref[...], 1, 1).astype(BF16).astype(F32)

    minus = jnp.full((tokens, width), -1.0, BF16)
    for window in range(count):
        span = slice(window * tokens, (window + 1) * tokens)
        state = states[window]
        query = state["q"][...]
        keys = state["k"][...].astype(F32)
        value = jnp.concatenate([state["v"][...], minus], 1)
        scaled = (grad_heads[span, :] * state["inverse"][...]).astype(BF16).astype(F32)
        inside = scaled * state["out"][...]
        inside_high = inside.astype(BF16).astype(F32)
        inside_low = pltpu.roll(inside - inside_high, head_size, 1)
        query_t = query.T.astype(BF16)
        scaled_t = scaled.T.astype(BF16)
        grad_k, grad_v, sources = [], [], []
        for head in range(heads):
            rows = slice(head * tokens, (head + 1) * tokens)
            part = slice(head * head_size, (head + 1) * head_size)
            extra = jnp.where(
                lane_head == head,
                inside_high,
                jnp.where(lane_head == (head + 1) % heads, inside_low, 0.0),
            ).astype(BF16)
            grad_weights = dot(jnp.concatenate([of_head(scaled, head, head_size), extra], 1), value, 1, 1)
            weights = state["p"][:, rows]
            grad_scores = grad_weights * weights.astype(F32)
            if window == 0:
                ds_ref[rows, :] = grad_scores
            else:
                ds_ref[rows, :] += grad_scores
            narrow = grad_scores.astype(BF16)
            dsn_ref[:, rows] = narrow
            sources.append(of_head(keys, head, head_size))
            grad_k.append(dot(query_t[part, :], narrow, 1, 0))
            grad_v.append(dot(scaled_t[part, :], weights, 1, 0))
        grad_q = dot(dsn_ref[...], jnp.concatenate(sources, 0), 1, 0)
        dqkv_ref[span, :width] = (grad_q * score_scale).astype(BF16)
        grad_k = jnp.concatenate(grad_k, 0).T
        dqkv_ref[span, width : 2 * width] = (grad_k * score_scale).astype(BF16)
        dqkv_ref[span, 2 * width :] = jnp.concatenate(grad_v, 0).T.astype(BF16)

    grad_projected = dqkv_ref[...]
    grad_qkv = dot(stacked("n"), grad_projected, 0, 0)
    for part in range(3):
        put(2 * hidden_units + part * width, grad_qkv[:, part * width : (part + 1) * width])
    grad_normed = dot(grad_projected, qkv_ref[...], 1, 1).astype(BF16).astype(F32)
    unit1 = stacked("unit")
    grad_gain1 = jnp.sum(grad_normed * unit1, axis=0, keepdims=True)
    grad_x = grad_hidden + norm_back(grad_normed * gain1_ref[...], unit1, stacked("scale"))
    gains = jnp.concatenate([grad_gain1, grad_gain2, jnp.zeros((6, width), F32)], 0)

    lanes = 2 * tokens
    rows = heads * WIN
    blank = jnp.zeros((WIN, LANES), F32)
    strip = jnp.zeros((rows, lanes), F32)
    for fine in range(8):
        near, far = WIN - 1 - fine, WIN - 9 - fine
        blocks = []
        for head in range(heads):
            above = ds_ref[head * tokens + near * WIN : head * tokens + (near + 1) * WIN, :]
            under = ds_ref[head * tokens + far * WIN : head * tokens + (far + 1) * WIN, :]
            blocks.append(
                jnp.concatenate([above, blank, blank], 1) + jnp.concatenate([blank, under, blank], 1)
            )
        block = jnp.concatenate(blocks, 0)
        strip = strip + (pltpu.roll(block, WIN * fine, 1) if fine else block)

    finish_table(heads, strip, grads_ref, 2 * hidden_units + 4 * width)
    row = 2 * hidden_units + 4 * width + heads * 2 * WIN
    blank = jnp.zeros((grads_ref.shape[0] - row - 8, width), F32)
    grads_ref[row:, :] = jnp.concatenate([gains, blank], 0).astype(BF16)
    half = keep_out.shape[0]
    core = lax.axis_index("group") % 2
    keep_out[...] = grads_ref[pl.ds(pl.multiple_of(core * half, 16), half), :]
    send_out[...] = grads_ref[pl.ds(pl.multiple_of((1 - core) * half, 16), half), :]

    for index, values in enumerate((out_ref[...], grad_x)):
        for window in range(count):
            start = WIN * window
            block = values[window * tokens : (window + 1) * tokens, :].reshape(WIN, WIN, width)
            top, low = block[:SHIFT], block[SHIFT:]
            if window == count - 1:
                own_out[index, :, start:, :] = low[:, SHIFT:].astype(BF16)
                below_out[index, :, start:, :] = top[:, SHIFT:].astype(BF16)
                right_out[index] = low[:, :SHIFT].astype(BF16)
                diag_out[index] = top[:, :SHIFT].astype(BF16)
            else:
                own_out[index, :, start : start + WIN, :] = low.astype(BF16)
                below_out[index, :, start : start + WIN, :] = top.astype(BF16)


def finish_table(heads, strip, grads_ref, row):
    rows, lanes = strip.shape
    lane = iota((rows, lanes), 1)
    amounts = WIN - 1 - iota((rows, lanes), 0) % WIN
    offsets = 2 * WIN
    table = jnp.zeros((heads * offsets, LANES), F32)
    for odd in range(2):
        chosen = jnp.where((lane // WIN) % 2 == odd, strip, 0.0)
        if odd:
            chosen = pltpu.roll(chosen, lanes - WIN, 1)
        chosen = shift_rows(chosen, amounts, True)
        wanted = offsets - 2 - iota((offsets, lanes), 0)
        where_row = (iota((offsets, lanes), 1) // 32) * 2 + odd == wanted
        terms = []
        for head in range(heads):
            flat = jnp.sum(chosen[head * WIN : (head + 1) * WIN, :], axis=0, keepdims=True)
            terms.append(jnp.where(where_row, flat, 0.0))
        terms = jnp.concatenate(terms, 0).astype(BF16)
        pick_lane = iota((lanes, LANES), 0) % 32
        pick = jnp.where(pick_lane == offsets - 2 - iota((lanes, LANES), 1), 1.0, 0.0).astype(BF16)
        table = table + dot(terms, pick, 1, 0)
    grads_ref[row : row + heads * offsets, :] = table.astype(BF16)


def pair_kernel(first_ref, second_ref, out_ref):
    total = first_ref[...].astype(F32) + second_ref[...].astype(F32)
    out_ref[...] = total.astype(out_ref.dtype)


def sum_kernel(in_ref, out_ref):
    total = in_ref[0].astype(F32)
    for index in range(1, in_ref.shape[0]):
        total = total + in_ref[index].astype(F32)
    total = total.astype(out_ref.dtype)
    for index in range(out_ref.shape[0]):
        out_ref[index] = total


def unpack_kernel(
    heads,
    factor,
    mine_ref,
    other_ref,
    diag_ref,
    above_ref,
    left_ref,
    own_ref,
    out_ref,
    grad_ref,
    gain1_ref,
    qkv_ref,
    proj_ref,
    table_ref,
    gain2_ref,
    fc1_ref,
    fc2_ref,
    summed_ref,
):
    width, hidden_units = fc1_ref.shape
    half = mine_ref.shape[0]
    early = own_ref.shape[2] - SHIFT
    cuts = ((slice(0, SHIFT), slice(early, None)), (slice(SHIFT, SHIFT + early), slice(0, early)))
    for index, target in enumerate((out_ref, grad_ref)):
        for cols, source in cuts:
            target[:SHIFT, cols, :] = own_ref[index, :, source, :]
            target[SHIFT:, cols, :] = above_ref[index, :, source, :]
        target[:SHIFT, SHIFT + early :, :] = left_ref[index]
        target[SHIFT:, SHIFT + early :, :] = diag_ref[index]
    core = lax.axis_index("group") % 2
    summed_ref[pl.ds(pl.multiple_of(core * half, 16), half), :] = mine_ref[...]
    summed_ref[pl.ds(pl.multiple_of((1 - core) * half, 16), half), :] = other_ref[...]
    offsets = 2 * WIN

    def rows(start, count):
        return summed_ref[start : start + count, :].astype(F32) * factor

    for part in range(hidden_units // width):
        fc1_ref[:, part * width : (part + 1) * width] = rows(part * width, width)
    fc2_ref[...] = rows(hidden_units, hidden_units)
    for part in range(3):
        qkv_ref[:, part * width : (part + 1) * width] = rows(2 * hidden_units + part * width, width)
    start = 2 * hidden_units + 3 * width
    proj_ref[...] = rows(start, width)
    start = start + width
    for head in range(heads):
        block = rows(start + head * offsets, offsets)
        table_ref[:, head, :] = block[: offsets - 1, : offsets - 1]
    start = start + heads * offsets
    gains = rows(start, 16)
    gain1_ref[...] = gains[0:1]
    gain2_ref[...] = gains[1:2]


def neighbour_pairs(row_step, col_step):
    groups, tiles = lax.axis_size("group"), lax.axis_size("tile")
    pairs = []
    for group in range(groups):
        for tile in range(tiles):
            target = ((group + row_step) % groups) * tiles + (tile + col_step) % tiles
            pairs.append((group * tiles + tile, target))
    return pairs


def passed_along(value, row_step, col_step):
    return lax.ppermute(value, AXES, neighbour_pairs(row_step, col_step))


def shards(tokens, gain1, w_qkv, w_proj, bias_table, gain2, w_fc1, w_fc2, cotangent):
    row_count, col_count, width = tokens.shape
    heads = bias_table.shape[0]
    hidden_units = w_fc1.shape[1]
    groups, tiles = lax.axis_size("group"), lax.axis_size("tile")
    devices = groups * tiles
    windows = col_count // WIN
    token_count = WIN * WIN
    keep = col_count - SHIFT

    vmem = pl.BlockSpec(memory_space=pltpu.VMEM)

    def array(shape, dtype=BF16):
        return jax.ShapeDtypeStruct(shape, dtype)

    table = bias_table.transpose(1, 0, 2)
    hbm = pl.BlockSpec(memory_space=pltpu.HBM)
    below, right, diag, table = pl.pallas_call(
        cut_kernel,
        out_shape=(
            array((2, SHIFT, keep, width)),
            array((2, SHIFT, SHIFT, width)),
            array((2, SHIFT, SHIFT, width)),
            array(table.shape, F32),
        ),
        in_specs=[hbm] * 3,
        out_specs=(vmem,) * 4,
        scratch_shapes=[pltpu.SemaphoreType.DMA((7,))],
        name="cut",
        compiler_params=PARAMS,
    )(*(pltpu.with_memory_space_constraint(each, pltpu.HBM) for each in (tokens, cotangent, table)))
    below = passed_along(below, 1, 0)
    right = passed_along(right, 0, 1)
    diag = passed_along(diag, 1, 1)

    bias = pl.pallas_call(
        functools.partial(bias_kernel, heads, windows),
        out_shape=jax.ShapeDtypeStruct((windows, heads * token_count, token_count), F32),
        in_specs=[vmem],
        out_specs=vmem,
        scratch_shapes=[pltpu.VMEM((heads * 2 * WIN, LANES), F32)],
        name="bias",
        compiler_params=PARAMS,
        cost_estimate=pl.CostEstimate(flops=8_000_000, bytes_accessed=2_000_000, transcendentals=0),
    )(table)

    used = 2 * hidden_units + 4 * width + heads * 2 * WIN + 16
    members = devices // 2
    chunk = (used + devices * 8 - 1) // (devices * 8) * 8
    half = chunk * members
    weights = (gain1.reshape(1, width), w_qkv, w_proj, gain2.reshape(1, width), w_fc1, w_fc2)
    total = windows * token_count
    state_types = dict.fromkeys(STATE, ((token_count, width), F32))
    state_types["scale"] = ((token_count, 1), F32)
    for name in ("n", "k", "v", "att"):
        state_types[name] = ((token_count, width), BF16)
    state_types["p"] = ((token_count, heads * token_count), BF16)
    states = pl.pallas_call(
        functools.partial(early_kernel, heads, windows),
        out_shape=[array(*state_types[name]) for name in STATE] * (windows - 1),
        in_specs=[vmem] * 5,
        out_specs=[vmem] * (len(STATE) * (windows - 1)),
        name="early",
        compiler_params=PARAMS,
        cost_estimate=pl.CostEstimate(
            flops=500_000_000, bytes_accessed=2_000_000, transcendentals=500_000
        ),
    )(tokens, below, bias, weights[0], w_qkv)
    inputs = (tokens, cotangent, below, right, diag, bias) + weights + tuple(states)
    own_out, below_out, right_out, diag_out, kept, sent = pl.pallas_call(
        functools.partial(block_kernel, heads, windows),
        out_shape=(
            array((2, SHIFT, keep, width)),
            array((2, SHIFT, keep, width)),
            array((2, SHIFT, SHIFT, width)),
            array((2, SHIFT, SHIFT, width)),
            array((half, width)),
            array((half, width)),
        ),
        in_specs=[vmem] * len(inputs),
        out_specs=(vmem,) * 6,
        scratch_shapes=[
            pltpu.VMEM((2 * half, width), BF16),
            pltpu.VMEM((total, width), BF16),
            pltpu.VMEM((total, 3 * width), BF16),
            pltpu.VMEM((heads * token_count, token_count), F32),
            pltpu.VMEM((token_count, heads * token_count), BF16),
            pltpu.VMEM((total, hidden_units), BF16),
            pltpu.VMEM((total, hidden_units), BF16),
            pltpu.VMEM((total, width), F32),
        ]
        + [pltpu.VMEM(*state_types[name]) for name in STATE],
        name="block",
        compiler_params=PARAMS,
        cost_estimate=pl.CostEstimate(
            flops=1_500_000_000, bytes_accessed=2_000_000, transcendentals=1_000_000
        ),
    )(*inputs)
    back_right = passed_along(right_out, 0, -1)
    back_diag = passed_along(diag_out, -1, -1)
    back_below = passed_along(below_out, -1, 0)

    pairs = [(index, index + tiles if index // tiles % 2 == 0 else index - tiles) for index in range(devices)]
    same_core = [
        [index for index in range(devices) if index // tiles % 2 == core] for core in range(2)
    ]

    def exchanged(value):
        return lax.all_to_all(value, AXES, 0, 0, tiled=True, axis_index_groups=same_core)

    received = lax.ppermute(sent, AXES, pairs)
    paired = pl.pallas_call(
        pair_kernel,
        out_shape=jax.ShapeDtypeStruct((half, width), BF16),
        in_specs=[vmem] * 2,
        out_specs=vmem,
        name="pair",
        compiler_params=PARAMS,
    )(kept, received)
    copies = pl.pallas_call(
        sum_kernel,
        out_shape=jax.ShapeDtypeStruct((members, chunk, width), BF16),
        in_specs=[vmem],
        out_specs=vmem,
        name="add",
        compiler_params=PARAMS,
    )(exchanged(paired.reshape(members, chunk, width)))
    mine = exchanged(copies).reshape(half, width)
    other = lax.ppermute(mine, AXES, pairs)

    factor = 1.0 / math.sqrt(row_count * groups * col_count * tiles)
    (
        block_output,
        grad_tokens,
        grad_gain1,
        grad_qkv,
        grad_proj,
        grad_table,
        grad_gain2,
        grad_fc1,
        grad_fc2,
    ) = pl.pallas_call(
        functools.partial(unpack_kernel, heads, factor),
        out_shape=(
            array(tokens.shape),
            array(tokens.shape),
            jax.ShapeDtypeStruct((1, width), F32),
            jax.ShapeDtypeStruct(w_qkv.shape, F32),
            jax.ShapeDtypeStruct(w_proj.shape, F32),
            jax.ShapeDtypeStruct((bias_table.shape[1], heads, bias_table.shape[2]), F32),
            jax.ShapeDtypeStruct((1, width), F32),
            jax.ShapeDtypeStruct(w_fc1.shape, F32),
            jax.ShapeDtypeStruct(w_fc2.shape, F32),
        ),
        in_specs=[vmem] * 6,
        out_specs=(vmem,) * 9,
        scratch_shapes=[pltpu.VMEM((2 * half, width), BF16)],
        name="unpack",
        compiler_params=PARAMS,
    )(mine, other, back_diag, back_below, back_right, own_out)

    return (
        block_output,
        grad_tokens,
        grad_gain1.reshape(width),
        grad_qkv,
        grad_proj,
        grad_table.transpose(1, 0, 2),
        grad_gain2.reshape(width),
        grad_fc1,
        grad_fc2,
    )


def solution(mesh):
    tile_spec = P("group", "tile", None)
    return jax.shard_map(
        shards,
        mesh=mesh,
        in_specs=(tile_spec, P(), P(), P(), P(), P(), P(), P(), tile_spec),
        out_specs=(tile_spec, tile_spec, P(), P(), P(), P(), P(), P(), P()),
        check_vma=False,
    )
```

```python
import functools
import math

import jax
import jax.numpy as jnp
from jax import lax
from jax.experimental import pallas as pl
from jax.experimental.pallas import tpu as pltpu
from jax.sharding import PartitionSpec as P


WIN = 16
SHIFT = 8
NORM_EPS = 1e-05
LOG2_E = math.log2(math.e)
LANES = 128
F32 = jnp.float32
BF16 = jnp.bfloat16
AXES = ("group", "tile")
PARAMS = pltpu.CompilerParams(vmem_limit_bytes=24 * 1024 * 1024)


def dot(left, right, left_dim, right_dim, precision=None):
    return lax.dot_general(
        left,
        right,
        (((left_dim,), (right_dim,)), ((), ())),
        preferred_element_type=F32,
        precision=precision,
    )


def iota(shape, dim):
    return lax.broadcasted_iota(jnp.int32, shape, dim)


def shift_rows(values, amounts, right):
    width = values.shape[1]
    for bit in range(4):
        step = 1 << bit
        moved = pltpu.roll(values, step if right else width - step, 1)
        values = jnp.where((amounts & step) != 0, moved, values)
    return values


def bias_kernel(heads, windows, table_ref, out_ref, pad_ref):
    span = 2 * WIN * WIN
    tokens = WIN * WIN
    offsets = 2 * WIN - 1
    block = offsets + 1
    pad_ref[...] = jnp.zeros_like(pad_ref)
    for head in range(heads):
        pad_ref[head * block : head * block + offsets, :offsets] = table_ref[:, head, :]
    padded = pad_ref[...]
    parts = []
    for _ in range(3):
        part = padded.astype(BF16)
        parts.append(part)
        padded = padded - part.astype(F32)
    chosen = iota((LANES, span), 1) % 32 == offsets - 1 - iota((LANES, span), 0)
    spread = dot(jnp.concatenate(parts, 0), jnp.where(chosen, 1.0, 0.0).astype(BF16), 1, 0)
    size = heads * block
    spread = spread[:size] + spread[size : 2 * size] + spread[2 * size :]
    flats = []
    for odd in range(2):
        wanted = offsets - 1 - iota((block, span), 0)
        keep = (iota((block, span), 1) // 32) * 2 + odd == wanted
        for head in range(heads):
            mine = spread[head * block : (head + 1) * block]
            flat = jnp.sum(jnp.where(keep, mine, 0.0), axis=0, keepdims=True)
            flats.append(jnp.broadcast_to(flat, (WIN, span)))
    rows = heads * WIN
    amounts = WIN - 1 - iota((rows, span), 0) % WIN
    even = shift_rows(jnp.concatenate(flats[:heads], 0), amounts, False)
    odd = shift_rows(jnp.concatenate(flats[heads:], 0), amounts, False)
    odd = pltpu.roll(odd, WIN, 1)
    strip = jnp.where(iota((rows, span), 1) % 32 < WIN, even, odd) * LOG2_E
    last_row = (lax.axis_index("group") == 0).astype(jnp.int32)
    last_col = (lax.axis_index("tile") == 0).astype(jnp.int32)
    key = iota((WIN, tokens), 1)
    query_x = iota((WIN, tokens), 0)
    key_low = (key >= tokens // 2).astype(jnp.int32)
    cross_col = ((key % WIN >= SHIFT) != (query_x >= SHIFT)).astype(jnp.int32)
    for fine in range(8):
        moved = pltpu.roll(strip, (span - WIN * fine) % span, 1)
        for coarse in range(2):
            y = WIN - 1 - (8 * coarse + fine)
            cross_row = key_low if y < SHIFT else 1 - key_low
            for window in range(windows):
                apart = cross_row * last_row
                if window == windows - 1:
                    apart = apart + cross_col * last_col
                extra = jnp.where(apart > 0, -1e30, 0.0)
                for head in range(heads):
                    part = moved[
                        head * WIN : (head + 1) * WIN,
                        LANES * coarse : LANES * coarse + tokens,
                    ]
                    start = head * tokens + y * WIN
                    out_ref[window, start : start + WIN, :] = part + extra


def mean_of(values):
    return jnp.mean(values, axis=-1, keepdims=True)


def norm(values):
    centred = values - mean_of(values)
    scale = lax.rsqrt(mean_of(centred * centred) + NORM_EPS)
    return centred * scale, scale


def norm_back(grad, unit, scale):
    return scale * (grad - mean_of(grad) - unit * mean_of(grad * unit))


def cut_kernel(token_ref, cot_ref, table_ref, below_ref, right_ref, diag_ref, table_out, sems):
    copies = []

    def copy(source, target):
        copies.append(pltpu.make_async_copy(source, target, sems.at[len(copies)]))

    keep = token_ref.shape[1] - SHIFT
    high, low = pl.ds(0, SHIFT), pl.ds(SHIFT, SHIFT)
    most, rest = pl.ds(0, keep), pl.ds(keep, SHIFT)
    for index, tile_ref in enumerate((token_ref, cot_ref)):
        copy(tile_ref.at[low, most], below_ref.at[index])
        copy(tile_ref.at[high, rest], right_ref.at[index])
        copy(tile_ref.at[low, rest], diag_ref.at[index])
    copy(table_ref, table_out)
    for each in copies:
        each.start()
    for each in copies:
        each.wait()


STATE = ("x", "n", "unit", "scale", "q", "k", "v", "p", "att", "out", "inverse")


def assemble(tile_ref, piece_refs, index, window, windows):
    tile = tile_ref[...].astype(F32)
    above = piece_refs[0][index].astype(F32)
    cols = slice(WIN * window + SHIFT, WIN * window + SHIFT + WIN)
    if window == windows - 1:
        left = piece_refs[1][index].astype(F32)
        diag = piece_refs[2][index].astype(F32)
        top = jnp.concatenate([diag, above[:, :SHIFT]], 1)
        low = jnp.concatenate([left, tile[:SHIFT, :SHIFT]], 1)
    else:
        top = above[:, cols]
        low = tile[:SHIFT, cols]
    return jnp.concatenate([top, low], 0).reshape(WIN * WIN, tile.shape[2])


def of_head(values, head, head_size):
    lane_head = iota((1, values.shape[1]), 1) // head_size
    return jnp.where(lane_head == head, values, 0.0).astype(BF16)


def attend(heads, window, bias_ref, gain1_ref, qkv_ref, state):
    tokens, width = state["x"].shape
    head_size = width // heads
    unit, scale = norm(state["x"][...])
    state["unit"][...] = unit
    state["scale"][...] = scale
    normed = (unit * gain1_ref[...]).astype(BF16)
    state["n"][...] = normed
    projected = dot(normed, qkv_ref[...], 1, 0)
    state["q"][...] = projected[:, :width]
    state["k"][...] = projected[:, width : 2 * width].astype(BF16)
    state["v"][...] = projected[:, 2 * width :].astype(BF16)
    query = state["q"][...]
    keys = state["k"][...]
    value = state["v"][...].astype(F32)
    sources = []
    for head in range(heads):
        rows = slice(head * tokens, (head + 1) * tokens)
        scores = dot(of_head(query, head, head_size), keys, 1, 1) * (head_size ** (-0.5) * LOG2_E)
        scores = scores + bias_ref[window, rows, :]
        weights = jnp.exp2(scores - jnp.max(scores, axis=-1, keepdims=True))
        state["p"][:, rows] = weights.astype(BF16)
        ones = jnp.broadcast_to(of_head(jnp.ones((1, width), F32), head, head_size), (tokens, width))
        sources.append(jnp.concatenate([of_head(value, head, head_size), ones], 1))
    both = dot(state["p"][...], jnp.concatenate(sources, 0), 1, 0)
    inverse = 1.0 / both[:, width:]
    attended = both[:, :width] * inverse
    state["inverse"][...] = inverse
    state["out"][...] = attended
    state["att"][...] = attended.astype(BF16)


def early_kernel(heads, windows, token_ref, below_ref, bias_ref, gain1_ref, qkv_ref, *refs):
    for window in range(windows - 1):
        state = dict(zip(STATE, refs[window * len(STATE) : (window + 1) * len(STATE)]))
        state["x"][...] = assemble(token_ref, (below_ref,), 0, window, windows)
        attend(heads, window, bias_ref, gain1_ref, qkv_ref, state)


def block_kernel(heads, windows, *refs):
    token_ref, cot_ref, below_ref, right_ref, diag_ref = refs[:5]
    bias_ref, gain1_ref, qkv_ref, proj_ref, gain2_ref, fc1_ref, fc2_ref = refs[5:12]
    refs = refs[12:]
    states = []
    for _ in range(windows - 1):
        states.append(dict(zip(STATE, refs)))
        refs = refs[len(STATE) :]
    own_out, below_out, right_out, diag_out, keep_out, send_out = refs[:6]
    grads_ref, c_ref, dqkv_ref, ds_ref, dsn_ref, inner_ref, before_ref, out_ref = refs[6:14]
    states.append(dict(zip(STATE, refs[14:])))
    count = windows

    tokens = WIN * WIN
    width = token_ref.shape[2]
    head_size = width // heads
    hidden_units = fc1_ref.shape[1]
    score_scale = head_size ** (-0.5)
    lane_head = iota((1, width), 1) // head_size
    pieces = (below_ref, right_ref, diag_ref)

    def put(row, value):
        grads_ref[row : row + value.shape[0], :] = value.astype(BF16)

    def stacked(name):
        return jnp.concatenate([state[name][...] for state in states], 0)

    states[-1]["x"][...] = assemble(token_ref, pieces, 0, windows - 1, windows)
    for window in range(windows):
        piece = assemble(cot_ref, pieces, 1, window, windows)
        c_ref[window * tokens : (window + 1) * tokens, :] = piece.astype(BF16)
    attend(heads, windows - 1, bias_ref, gain1_ref, qkv_ref, states[-1])

    attended = stacked("att")
    hidden = stacked("x") + dot(attended, proj_ref[...], 1, 0).astype(BF16).astype(F32)
    unit2, scale2 = norm(hidden)
    normed2 = (unit2 * gain2_ref[...]).astype(BF16)
    cot = c_ref[...]
    root = math.sqrt(0.5)
    step = 2 * width
    for part in range(hidden_units // step):
        cols = slice(part * step, (part + 1) * step)
        before = dot(normed2, fc1_ref[:, cols], 1, 0)
        normal = 0.5 * (1.0 + lax.erf(before * root))
        inner_ref[:, cols] = (before * normal).astype(BF16)
        density = jnp.exp2(before * before * (-0.5 * LOG2_E)) * (1.0 / math.sqrt(2.0 * math.pi))
        slope = normal + before * density
        grad_inner = dot(cot, fc2_ref[cols, :], 1, 1).astype(BF16).astype(F32)
        before_ref[:, cols] = (grad_inner * slope).astype(BF16)
    inner = inner_ref[...]
    grad_before = before_ref[...]
    out_ref[...] = hidden + dot(inner, fc2_ref[...], 1, 0)
    back = dot(grad_before, fc1_ref[...], 1, 1).astype(BF16).astype(F32)
    grad_fc1 = dot(normed2, grad_before, 0, 0)
    for part in range(hidden_units // width):
        put(part * width, grad_fc1[:, part * width : (part + 1) * width])
    put(hidden_units, dot(inner, cot, 0, 0))
    grad_gain2 = jnp.sum(back * unit2, axis=0, keepdims=True)
    grad_hidden = cot.astype(F32) + norm_back(back * gain2_ref[...], unit2, scale2)

    grad_attended = grad_hidden.astype(BF16)
    put(2 * hidden_units + 3 * width, dot(attended, grad_attended, 0, 0))
    grad_heads = dot(grad_attended, proj_ref[...], 1, 1).astype(BF16).astype(F32)

    minus = jnp.full((tokens, width), -1.0, BF16)
    for window in range(count):
        span = slice(window * tokens, (window + 1) * tokens)
        state = states[window]
        query = state["q"][...]
        keys = state["k"][...].astype(F32)
        value = jnp.concatenate([state["v"][...], minus], 1)
        scaled = (grad_heads[span, :] * state["inverse"][...]).astype(BF16).astype(F32)
        inside = scaled * state["out"][...]
        inside_high = inside.astype(BF16).astype(F32)
        inside_low = pltpu.roll(inside - inside_high, head_size, 1)
        query_t = query.T.astype(BF16)
        scaled_t = scaled.T.astype(BF16)
        grad_k, grad_v, sources = [], [], []
        for head in range(heads):
            rows = slice(head * tokens, (head + 1) * tokens)
            part = slice(head * head_size, (head + 1) * head_size)
            extra = jnp.where(
                lane_head == head,
                inside_high,
                jnp.where(lane_head == (head + 1) % heads, inside_low, 0.0),
            ).astype(BF16)
            grad_weights = dot(jnp.concatenate([of_head(scaled, head, head_size), extra], 1), value, 1, 1)
            weights = state["p"][:, rows]
            grad_scores = grad_weights * weights.astype(F32)
            if window == 0:
                ds_ref[rows, :] = grad_scores
            else:
                ds_ref[rows, :] += grad_scores
            narrow = grad_scores.astype(BF16)
            dsn_ref[:, rows] = narrow
            sources.append(of_head(keys, head, head_size))
            grad_k.append(dot(query_t[part, :], narrow, 1, 0))
            grad_v.append(dot(scaled_t[part, :], weights, 1, 0))
        grad_q = dot(dsn_ref[...], jnp.concatenate(sources, 0), 1, 0)
        dqkv_ref[span, :width] = (grad_q * score_scale).astype(BF16)
        grad_k = jnp.concatenate(grad_k, 0).T
        dqkv_ref[span, width : 2 * width] = (grad_k * score_scale).astype(BF16)
        dqkv_ref[span, 2 * width :] = jnp.concatenate(grad_v, 0).T.astype(BF16)

    grad_projected = dqkv_ref[...]
    grad_qkv = dot(stacked("n"), grad_projected, 0, 0)
    for part in range(3):
        put(2 * hidden_units + part * width, grad_qkv[:, part * width : (part + 1) * width])
    grad_normed = dot(grad_projected, qkv_ref[...], 1, 1).astype(BF16).astype(F32)
    unit1 = stacked("unit")
    grad_gain1 = jnp.sum(grad_normed * unit1, axis=0, keepdims=True)
    grad_x = grad_hidden + norm_back(grad_normed * gain1_ref[...], unit1, stacked("scale"))
    gains = jnp.concatenate([grad_gain1, grad_gain2, jnp.zeros((6, width), F32)], 0)

    lanes = 2 * tokens
    rows = heads * WIN
    blank = jnp.zeros((WIN, LANES), F32)
    strip = jnp.zeros((rows, lanes), F32)
    for fine in range(8):
        near, far = WIN - 1 - fine, WIN - 9 - fine
        blocks = []
        for head in range(heads):
            above = ds_ref[head * tokens + near * WIN : head * tokens + (near + 1) * WIN, :]
            under = ds_ref[head * tokens + far * WIN : head * tokens + (far + 1) * WIN, :]
            blocks.append(
                jnp.concatenate([above, blank, blank], 1) + jnp.concatenate([blank, under, blank], 1)
            )
        block = jnp.concatenate(blocks, 0)
        strip = strip + (pltpu.roll(block, WIN * fine, 1) if fine else block)

    finish_table(heads, strip, grads_ref, 2 * hidden_units + 4 * width)
    row = 2 * hidden_units + 4 * width + heads * 2 * WIN
    blank = jnp.zeros((grads_ref.shape[0] - row - 8, width), F32)
    grads_ref[row:, :] = jnp.concatenate([gains, blank], 0).astype(BF16)
    half = keep_out.shape[0]
    core = lax.axis_index("group") % 2
    keep_out[...] = grads_ref[pl.ds(pl.multiple_of(core * half, 16), half), :]
    send_out[...] = grads_ref[pl.ds(pl.multiple_of((1 - core) * half, 16), half), :]

    for index, values in enumerate((out_ref[...], grad_x)):
        for window in range(count):
            start = WIN * window
            block = values[window * tokens : (window + 1) * tokens, :].reshape(WIN, WIN, width)
            top, low = block[:SHIFT], block[SHIFT:]
            if window == count - 1:
                own_out[index, :, start:, :] = low[:, SHIFT:].astype(BF16)
                below_out[index, :, start:, :] = top[:, SHIFT:].astype(BF16)
                right_out[index] = low[:, :SHIFT].astype(BF16)
                diag_out[index] = top[:, :SHIFT].astype(BF16)
            else:
                own_out[index, :, start : start + WIN, :] = low.astype(BF16)
                below_out[index, :, start : start + WIN, :] = top.astype(BF16)


def finish_table(heads, strip, grads_ref, row):
    rows, lanes = strip.shape
    lane = iota((rows, lanes), 1)
    amounts = WIN - 1 - iota((rows, lanes), 0) % WIN
    offsets = 2 * WIN
    table = jnp.zeros((heads * offsets, LANES), F32)
    for odd in range(2):
        chosen = jnp.where((lane // WIN) % 2 == odd, strip, 0.0)
        if odd:
            chosen = pltpu.roll(chosen, lanes - WIN, 1)
        chosen = shift_rows(chosen, amounts, True)
        wanted = offsets - 2 - iota((offsets, lanes), 0)
        where_row = (iota((offsets, lanes), 1) // 32) * 2 + odd == wanted
        terms = []
        for head in range(heads):
            flat = jnp.sum(chosen[head * WIN : (head + 1) * WIN, :], axis=0, keepdims=True)
            terms.append(jnp.where(where_row, flat, 0.0))
        terms = jnp.concatenate(terms, 0).astype(BF16)
        pick_lane = iota((lanes, LANES), 0) % 32
        pick = jnp.where(pick_lane == offsets - 2 - iota((lanes, LANES), 1), 1.0, 0.0).astype(BF16)
        table = table + dot(terms, pick, 1, 0)
    grads_ref[row : row + heads * offsets, :] = table.astype(BF16)


def pair_kernel(first_ref, second_ref, out_ref):
    total = first_ref[...].astype(F32) + second_ref[...].astype(F32)
    out_ref[...] = total.astype(out_ref.dtype)


def sum_kernel(in_ref, out_ref):
    total = in_ref[0].astype(F32)
    for index in range(1, in_ref.shape[0]):
        total = total + in_ref[index].astype(F32)
    total = total.astype(out_ref.dtype)
    for index in range(out_ref.shape[0]):
        out_ref[index] = total


def unpack_kernel(
    heads,
    factor,
    mine_ref,
    other_ref,
    gain1_ref,
    qkv_ref,
    proj_ref,
    table_ref,
    gain2_ref,
    fc1_ref,
    fc2_ref,
    summed_ref,
):
    width, hidden_units = fc1_ref.shape
    half = mine_ref.shape[0]
    core = lax.axis_index("group") % 2
    summed_ref[pl.ds(pl.multiple_of(core * half, 16), half), :] = mine_ref[...]
    summed_ref[pl.ds(pl.multiple_of((1 - core) * half, 16), half), :] = other_ref[...]
    offsets = 2 * WIN

    def rows(start, count):
        return summed_ref[start : start + count, :].astype(F32) * factor

    for part in range(hidden_units // width):
        fc1_ref[:, part * width : (part + 1) * width] = rows(part * width, width)
    fc2_ref[...] = rows(hidden_units, hidden_units)
    for part in range(3):
        qkv_ref[:, part * width : (part + 1) * width] = rows(2 * hidden_units + part * width, width)
    start = 2 * hidden_units + 3 * width
    proj_ref[...] = rows(start, width)
    start = start + width
    for head in range(heads):
        block = rows(start + head * offsets, offsets)
        table_ref[:, head, :] = block[: offsets - 1, : offsets - 1]
    start = start + heads * offsets
    gains = rows(start, 16)
    gain1_ref[...] = gains[0:1]
    gain2_ref[...] = gains[1:2]


def tiles_kernel(diag_ref, above_ref, left_ref, own_ref, out_ref, grad_ref):
    early = own_ref.shape[2] - SHIFT
    cuts = ((slice(0, SHIFT), slice(early, None)), (slice(SHIFT, SHIFT + early), slice(0, early)))
    for index, target in enumerate((out_ref, grad_ref)):
        for cols, source in cuts:
            target[:SHIFT, cols, :] = own_ref[index, :, source, :]
            target[SHIFT:, cols, :] = above_ref[index, :, source, :]
        target[:SHIFT, SHIFT + early :, :] = left_ref[index]
        target[SHIFT:, SHIFT + early :, :] = diag_ref[index]


def neighbour_pairs(row_step, col_step):
    groups, tiles = lax.axis_size("group"), lax.axis_size("tile")
    pairs = []
    for group in range(groups):
        for tile in range(tiles):
            target = ((group + row_step) % groups) * tiles + (tile + col_step) % tiles
            pairs.append((group * tiles + tile, target))
    return pairs


def passed_along(value, row_step, col_step):
    return lax.ppermute(value, AXES, neighbour_pairs(row_step, col_step))


def shards(tokens, gain1, w_qkv, w_proj, bias_table, gain2, w_fc1, w_fc2, cotangent):
    row_count, col_count, width = tokens.shape
    heads = bias_table.shape[0]
    hidden_units = w_fc1.shape[1]
    groups, tiles = lax.axis_size("group"), lax.axis_size("tile")
    devices = groups * tiles
    windows = col_count // WIN
    token_count = WIN * WIN
    keep = col_count - SHIFT

    vmem = pl.BlockSpec(memory_space=pltpu.VMEM)

    def array(shape, dtype=BF16):
        return jax.ShapeDtypeStruct(shape, dtype)

    table = bias_table.transpose(1, 0, 2)
    hbm = pl.BlockSpec(memory_space=pltpu.HBM)
    below, right, diag, table = pl.pallas_call(
        cut_kernel,
        out_shape=(
            array((2, SHIFT, keep, width)),
            array((2, SHIFT, SHIFT, width)),
            array((2, SHIFT, SHIFT, width)),
            array(table.shape, F32),
        ),
        in_specs=[hbm] * 3,
        out_specs=(vmem,) * 4,
        scratch_shapes=[pltpu.SemaphoreType.DMA((7,))],
        name="cut",
        compiler_params=PARAMS,
    )(*(pltpu.with_memory_space_constraint(each, pltpu.HBM) for each in (tokens, cotangent, table)))
    below = passed_along(below, 1, 0)
    right = passed_along(right, 0, 1)
    diag = passed_along(diag, 1, 1)

    bias = pl.pallas_call(
        functools.partial(bias_kernel, heads, windows),
        out_shape=jax.ShapeDtypeStruct((windows, heads * token_count, token_count), F32),
        in_specs=[vmem],
        out_specs=vmem,
        scratch_shapes=[pltpu.VMEM((heads * 2 * WIN, LANES), F32)],
        name="bias",
        compiler_params=PARAMS,
        cost_estimate=pl.CostEstimate(flops=8_000_000, bytes_accessed=2_000_000, transcendentals=0),
    )(table)

    used = 2 * hidden_units + 4 * width + heads * 2 * WIN + 16
    members = devices // 2
    chunk = (used + devices * 8 - 1) // (devices * 8) * 8
    half = chunk * members
    weights = (gain1.reshape(1, width), w_qkv, w_proj, gain2.reshape(1, width), w_fc1, w_fc2)
    total = windows * token_count
    state_types = dict.fromkeys(STATE, ((token_count, width), F32))
    state_types["scale"] = ((token_count, 1), F32)
    for name in ("n", "k", "v", "att"):
        state_types[name] = ((token_count, width), BF16)
    state_types["p"] = ((token_count, heads * token_count), BF16)
    states = pl.pallas_call(
        functools.partial(early_kernel, heads, windows),
        out_shape=[array(*state_types[name]) for name in STATE] * (windows - 1),
        in_specs=[vmem] * 5,
        out_specs=[vmem] * (len(STATE) * (windows - 1)),
        name="early",
        compiler_params=PARAMS,
        cost_estimate=pl.CostEstimate(
            flops=500_000_000, bytes_accessed=2_000_000, transcendentals=500_000
        ),
    )(tokens, below, bias, weights[0], w_qkv)
    inputs = (tokens, cotangent, below, right, diag, bias) + weights + tuple(states)
    own_out, below_out, right_out, diag_out, kept, sent = pl.pallas_call(
        functools.partial(block_kernel, heads, windows),
        out_shape=(
            array((2, SHIFT, keep, width)),
            array((2, SHIFT, keep, width)),
            array((2, SHIFT, SHIFT, width)),
            array((2, SHIFT, SHIFT, width)),
            array((half, width)),
            array((half, width)),
        ),
        in_specs=[vmem] * len(inputs),
        out_specs=(vmem,) * 6,
        scratch_shapes=[
            pltpu.VMEM((2 * half, width), BF16),
            pltpu.VMEM((total, width), BF16),
            pltpu.VMEM((total, 3 * width), BF16),
            pltpu.VMEM((heads * token_count, token_count), F32),
            pltpu.VMEM((token_count, heads * token_count), BF16),
            pltpu.VMEM((total, hidden_units), BF16),
            pltpu.VMEM((total, hidden_units), BF16),
            pltpu.VMEM((total, width), F32),
        ]
        + [pltpu.VMEM(*state_types[name]) for name in STATE],
        name="block",
        compiler_params=PARAMS,
        cost_estimate=pl.CostEstimate(
            flops=1_500_000_000, bytes_accessed=2_000_000, transcendentals=1_000_000
        ),
    )(*inputs)
    back_right = passed_along(right_out, 0, -1)
    back_diag = passed_along(diag_out, -1, -1)
    back_below = passed_along(below_out, -1, 0)

    pairs = [(index, index + tiles if index // tiles % 2 == 0 else index - tiles) for index in range(devices)]
    same_core = [
        [index for index in range(devices) if index // tiles % 2 == core] for core in range(2)
    ]

    def exchanged(value):
        return lax.all_to_all(value, AXES, 0, 0, tiled=True, axis_index_groups=same_core)

    received = lax.ppermute(sent, AXES, pairs)
    paired = pl.pallas_call(
        pair_kernel,
        out_shape=jax.ShapeDtypeStruct((half, width), BF16),
        in_specs=[vmem] * 2,
        out_specs=vmem,
        name="pair",
        compiler_params=PARAMS,
    )(kept, received)
    copies = pl.pallas_call(
        sum_kernel,
        out_shape=jax.ShapeDtypeStruct((members, chunk, width), BF16),
        in_specs=[vmem],
        out_specs=vmem,
        name="add",
        compiler_params=PARAMS,
    )(exchanged(paired.reshape(members, chunk, width)))
    mine = exchanged(copies).reshape(half, width)
    other = lax.ppermute(mine, AXES, pairs)

    factor = 1.0 / math.sqrt(row_count * groups * col_count * tiles)
    block_output, grad_tokens = pl.pallas_call(
        tiles_kernel,
        out_shape=(array(tokens.shape), array(tokens.shape)),
        in_specs=[vmem] * 4,
        out_specs=(vmem,) * 2,
        name="tiles",
        compiler_params=PARAMS,
        cost_estimate=pl.CostEstimate(flops=4_000_000, bytes_accessed=600_000, transcendentals=0),
    )(back_diag, back_below, back_right, own_out)
    (
        grad_gain1,
        grad_qkv,
        grad_proj,
        grad_table,
        grad_gain2,
        grad_fc1,
        grad_fc2,
    ) = pl.pallas_call(
        functools.partial(unpack_kernel, heads, factor),
        out_shape=(
            jax.ShapeDtypeStruct((1, width), F32),
            jax.ShapeDtypeStruct(w_qkv.shape, F32),
            jax.ShapeDtypeStruct(w_proj.shape, F32),
            jax.ShapeDtypeStruct((bias_table.shape[1], heads, bias_table.shape[2]), F32),
            jax.ShapeDtypeStruct((1, width), F32),
            jax.ShapeDtypeStruct(w_fc1.shape, F32),
            jax.ShapeDtypeStruct(w_fc2.shape, F32),
        ),
        in_specs=[vmem] * 2,
        out_specs=(vmem,) * 7,
        scratch_shapes=[pltpu.VMEM((2 * half, width), BF16)],
        name="unpack",
        compiler_params=PARAMS,
    )(mine, other)

    return (
        block_output,
        grad_tokens,
        grad_gain1.reshape(width),
        grad_qkv,
        grad_proj,
        grad_table.transpose(1, 0, 2),
        grad_gain2.reshape(width),
        grad_fc1,
        grad_fc2,
    )


def solution(mesh):
    tile_spec = P("group", "tile", None)
    return jax.shard_map(
        shards,
        mesh=mesh,
        in_specs=(tile_spec, P(), P(), P(), P(), P(), P(), P(), tile_spec),
        out_specs=(tile_spec, tile_spec, P(), P(), P(), P(), P(), P(), P()),
        check_vma=False,
    )
```
